32 devices in a mesh: occ: 8 (over y, x, core), frag: 4 (over z).
Axes of the slice: x: 2, y: 2, z: 4, core: 2. Of those that a mesh axis runs over, the one named last changes fastest.
Arguments:
- factors: bfloat16 [32, 512, 1280], P(('frag', 'occ')), parts along dimension 0, may hold values from -1 to 1
- occ_energy: float32 [32], P('frag'), parts along dimension 0, may hold values from -2 to -0.3
- vir_energy: float32 [2048], P('frag'), parts along dimension 0, may hold values from 0.2 to 4
- coeffs: bfloat16 [4096, 512], P('frag'), parts along dimension 0, may hold values from -0.25 to 0.25
Outputs:
- back: bfloat16 [1280, 32, 1024], P('occ', 'frag'), parts along dimension 1
The draws below stay inside these ranges and needn't reach their ends.
There are 4 independent parts, one for each index of `frag`. The reference program is written for one: setup_inputs(seed, part) draws one part's arguments, and reference() takes and returns one part's arrays. A program takes and returns all parts, laid end to end along the dimension named above; each array names one. Nothing has to cross between parts.
All inputs are finite; a program needn't handle non-finite values.
Results may differ from the reference program's by a relative error of at most 0.008.
Values may be sent and summed in bfloat16 or wider, within the bound.
A program may use at most 64 MiB of HBM per device.

```python
import jax
import jax.numpy as jnp
from jax import lax

V = 512
A = 1280
NAO = 1024
OFFSETS = 3
OCC = 8


def steps_of(own_key, extent, cuts, least, high):
    def one(position, shards_of):
        steps = jax.random.uniform(jax.random.fold_in(jax.random.fold_in(own_key, 6), position), (shards_of,), jnp.float32, least / len(cuts), high / len(cuts))
        return jnp.repeat(jnp.exp(steps), extent[position] // shards_of).reshape((-1,) + (1,) * (len(extent) - position - 1))

    loudness = one(*cuts[0])
    for cut in cuts[1:]:
        loudness = loudness * one(*cut)
    return loudness


def normal_values(own_key, extent, scale, bound, shards=(), held_as=jnp.bfloat16):
    gain = steps_of(own_key, extent, shards, -0.22, 0.18) if shards else 1.0
    array = jax.random.normal(own_key, extent, jnp.float32) * scale * gain
    return jnp.minimum(jnp.maximum(array, -bound), bound).astype(held_as)


def setup_inputs(seed: int = 0, part: int = 0) -> dict:
    seeds = jax.random.split(jax.random.key(seed), 5)
    own_keys = jax.random.split(jax.random.fold_in(seeds[4], part), 5)
    return {
        "factors": normal_values(own_keys[0], (OCC, V, A), 0.17, 1.0, ((0, 8),)),
        "occ_energy": jnp.clip(jax.random.uniform(own_keys[1], (OCC,), jnp.float32, -2.0, -0.3), -2.0, -0.3),
        "vir_energy": jnp.clip(jax.random.uniform(own_keys[2], (V,), jnp.float32, 0.2, 4.0), 0.2, 4.0),
        "coeffs": normal_values(own_keys[3], (NAO, V), V ** -0.5, 0.25),
    }


def rounded(value):
    return lax.optimization_barrier(value.astype(jnp.bfloat16)).astype(jnp.float32)


def reference(factors, occ_energy, vir_energy, coeffs):
    mine = factors.astype(jnp.float32)
    own = jnp.zeros((OCC, A, V), jnp.float32)
    incoming = jnp.zeros((OCC, A, V), jnp.float32)
    for offset in range(1, OFFSETS + 1):
        partner = jnp.roll(mine, -offset, axis=0)
        pair_energy = occ_energy + jnp.roll(occ_energy, -offset)
        kmat = jnp.einsum('iap,ibp->iab', mine, partner)
        denom = pair_energy[:, None, None] - vir_energy[None, :, None] - vir_energy[None, None, :]
        amps = rounded(kmat / denom)
        own = own + jnp.einsum('iab,ibp->ipa', amps, partner)
        sent = rounded(jnp.einsum('iap,iab->ipb', mine, amps))
        incoming = incoming + jnp.roll(sent, offset, axis=0)
    gamma = rounded(own + incoming)
    return jnp.einsum('ipa,ma->pim', gamma, coeffs.astype(jnp.float32)).astype(jnp.bfloat16)
```

```python
import jax
import jax.numpy as jnp
from jax import lax
from jax.experimental import pallas as pl
from jax.experimental.pallas import tpu as pltpu
from jax.sharding import PartitionSpec as P

OFFSETS = 3


def passed_along(block, axis, distance):
    devices = range(lax.axis_size(axis))
    route = [((i - distance) % len(devices), i) for i in devices]
    return lax.ppermute(block, axis, route)


def on_device(factors, occ_energy, vir_energy, coeffs):
    mine = factors[0]
    count = lax.axis_size("occ")
    index = lax.axis_index("occ")
    partners = []
    current = mine
    for offset in range(1, OFFSETS + 1):
        current = passed_along(current, "occ", -1)
        partners.append(current)
    own_energy = lax.dynamic_index_in_dim(occ_energy, index, 0, False)
    own = jnp.zeros((mine.shape[1], mine.shape[0]), jnp.float32)
    outgoing = []
    for offset in range(1, OFFSETS + 1):
        partner = partners[offset - 1]
        other_energy = lax.dynamic_index_in_dim(occ_energy, (index + offset) % count, 0, False)
        kmat = lax.dot_general(
            mine, partner, (((1,), (1,)), ((), ())), preferred_element_type=jnp.float32
        )
        denom = own_energy + other_energy - vir_energy[:, None] - vir_energy[None, :]
        amps = (kmat / denom).astype(jnp.bfloat16)
        own = own + lax.dot_general(
            partner, amps, (((0,), (1,)), ((), ())), preferred_element_type=jnp.float32
        )
        sent = lax.dot_general(
            mine, amps, (((0,), (0,)), ((), ())), preferred_element_type=jnp.float32
        )
        outgoing.append(sent.astype(jnp.bfloat16))
    incoming = jnp.zeros_like(own)
    for offset in range(1, OFFSETS + 1):
        arrived = passed_along(outgoing[offset - 1], "occ", offset)
        incoming = incoming + arrived.astype(jnp.float32)
    gamma = (own + incoming).astype(jnp.bfloat16)[None]
    slabs = lax.all_to_all(gamma, "occ", split_axis=1, concat_axis=0, tiled=True)
    return jnp.einsum("ipa,ma->pim", slabs, coeffs, preferred_element_type=jnp.float32).astype(
        jnp.bfloat16
    )


LANES = 128
ROWS = 128
CHUNK = ROWS // 2

LAG = 3
DEPTH = 2

SIDE = ((2, 0, 4), (2, 2, 4), (2, 0, 5), (2, 2, 5))


def flipped(a, b):
    bits = [(a // w % 2 + b // w % 2) % 2 * w for w in (1, 2, 4)]
    return bits[0] + bits[1] + bits[2]


def entry(table, column, n):
    packed = sum(row[column] << (3 * k) for k, row in enumerate(table))
    return lax.shift_right_logical(jnp.int32(packed), jnp.int32(3) * n) % 8


def gathered_kernel(
    mine_ref, energy_hbm, vir_hbm, out_ref,
    blocks, slabs, total, wide, pick, vcol, held_a, held_b, energy_ref, vir_ref,
    local_sem, small_sem, own_sem, fwd_sem, sib_sem, recv_sem, give_sem, take_sem,
):
    me = lax.axis_index("occ")
    parity = me % 2
    count = blocks.shape[0]
    virtuals, depth = mine_ref.shape
    width = total.shape[1]
    window = pick.shape[1]
    steps = virtuals // ROWS
    chunks = virtuals // CHUNK
    half = virtuals // 2
    first = me * width
    lead = pl.multiple_of(first // LANES * LANES, LANES)
    skip = first % LANES

    def rows_of(q):
        return pl.ds(pl.multiple_of(q * CHUNK, CHUNK), CHUNK)

    def local(q):
        return pltpu.make_async_copy(
            mine_ref.at[rows_of(q)], blocks.at[me, rows_of(q)], local_sem.at[q]
        )

    energy_copy = pltpu.make_async_copy(energy_hbm, energy_ref, small_sem.at[0])
    vir_copy = pltpu.make_async_copy(vir_hbm, vir_ref, small_sem.at[1])

    barrier = pltpu.get_barrier_semaphore()
    for bit in (1, 2, 4):
        pl.semaphore_signal(
            barrier, inc=1, device_id={"occ": flipped(me, bit)},
            device_id_type=pl.DeviceIdType.MESH,
        )

    @pl.loop(0, chunks)
    def _(q):
        local(q).start()

    energy_copy.start()
    vir_copy.start()
    pl.semaphore_wait(barrier, 3)

    def send(label, q, bit, send_sem):
        place = blocks.at[flipped(me, label), rows_of(q)]
        return pltpu.make_async_remote_copy(
            src_ref=place,
            dst_ref=place,
            send_sem=send_sem,
            recv_sem=recv_sem.at[flipped(label, bit), q],
            device_id={"occ": flipped(me, bit)},
            device_id_type=pl.DeviceIdType.MESH,
        )

    def own_send(q, axis):
        return send(0, q, 2 + 2 * axis, own_sem.at[axis, q])

    def far_send(q, label):
        return send(label, q, 6 - label, fwd_sem.at[q])

    def sib_send(q, label):
        return send(label, q, 1, sib_sem.at[label // 2, q])

    def arrived(label, q):
        place = blocks.at[flipped(me, label), rows_of(q)]
        pltpu.make_async_copy(place, place, recv_sem.at[label, q]).wait()

    def give(n):
        return pltpu.make_async_remote_copy(
            src_ref=held_a.at[n],
            dst_ref=held_b.at[n],
            send_sem=give_sem.at[n],
            recv_sem=take_sem.at[n],
            device_id={"occ": flipped(me, 1)},
            device_id_type=pl.DeviceIdType.MESH,
        )

    def taken(n):
        place = held_b.at[n]
        pltpu.make_async_copy(place, place, take_sem.at[n]).wait()

    def next_sends(q):
        @pl.when(q < chunks)
        def _():
            own_send(q, 0).start()
            own_send(q, 1).start()

        @pl.when(q >= chunks)
        def _():
            far_send(2 * (q - chunks), 2).start()
            far_send(2 * (q - chunks) + 1, 4).start()

    for q in range(DEPTH):
        local(q).wait()
        own_send(q, 0).start()
        own_send(q, 1).start()
        sib_send(q, 0).start()

    @pl.loop(DEPTH, chunks)
    def _(q):
        local(q).wait()
        sib_send(q, 0).start()

    energy_copy.wait()
    vir_copy.wait()
    total[...] = jnp.zeros_like(total)
    column = lax.broadcasted_iota(jnp.int32, (width, window), 1)
    row = lax.broadcasted_iota(jnp.int32, (width, window), 0)
    pick[...] = jnp.where(column == row + skip, 1.0, 0.0).astype(jnp.bfloat16)
    for t in range(steps):
        part = vir_ref[:, t * ROWS:(t + 1) * ROWS]
        vcol[t * ROWS:(t + 1) * ROWS, :] = jnp.broadcast_to(part, (ROWS, ROWS)).T

    def rows_at(t):
        return pl.ds(pl.multiple_of(t * ROWS, ROWS), ROWS)

    def turn_all(label):
        u = flipped(me, label)
        slabs[u] = lax.dot_general(
            pick[...], blocks[u, :, pl.ds(lead, window)], (((1,), (1,)), ((), ())),
            preferred_element_type=jnp.float32,
        ).astype(jnp.bfloat16)

    def turn(la, lb, t):
        ua, ub = flipped(me, la), flipped(me, lb)
        both = jnp.concatenate(
            [blocks[ua, rows_at(t), pl.ds(lead, window)], blocks[ub, rows_at(t), pl.ds(lead, window)]],
            axis=0,
        )
        moved = lax.dot_general(
            pick[...], both, (((1,), (1,)), ((), ())), preferred_element_type=jnp.float32
        ).astype(jnp.bfloat16)
        slabs[ua, :, rows_at(t)] = moved[:, :ROWS]
        slabs[ub, :, rows_at(t)] = moved[:, ROWS:]

    def amps_of(item, n):
        ua, ta, ub, tb, v = item
        some = jnp.concatenate([blocks[ua, rows_at(ta), :], blocks[ub, rows_at(tb), :]], axis=0)
        level = jnp.concatenate(
            [energy_ref[ua] - vir_ref[:, rows_at(ta)], energy_ref[ub] - vir_ref[:, rows_at(tb)]],
            axis=1,
        ) + energy_ref[v]
        for h in range(2):
            rows = slice(h * half, (h + 1) * half)
            kmat = lax.dot_general(
                blocks[v, rows, :], some, (((1,), (1,)), ((), ())),
                preferred_element_type=jnp.float32,
            )
            held_a[n, rows, :] = (kmat / (level - vcol[rows, 0:1])).astype(jnp.bfloat16)

    def gather(item, held):
        ua, ta, ub, tb, v = item
        left = jnp.concatenate([slabs[ua, :, rows_at(ta)], slabs[ub, :, rows_at(tb)]], axis=1)
        both = jnp.dot(slabs[v], held[...], preferred_element_type=jnp.float32)
        other = lax.dot_general(
            left, held[...], (((1,), (1,)), ((), ())), preferred_element_type=jnp.float32
        )
        total[ua, :, rows_at(ta)] += both[:, :ROWS]
        total[ub, :, rows_at(tb)] += both[:, ROWS:]
        total[v] += other

    def gather_both(pair, n):
        gather(pair[0], held_a.at[n])
        gather(pair[1], held_b.at[n])

    def placed(item):
        return (
            flipped(me, item[0]), jnp.int32(item[1]), flipped(me, item[2]), jnp.int32(item[3]),
            flipped(me, item[4]),
        )

    def mirrored(item):
        return (flipped(item[0], 1), item[1], flipped(item[2], 1), item[3], flipped(item[4], 1))

    def crossed(u, ta, w, tb, v):
        item = placed((u, ta, w, tb, v))
        return item, mirrored(item)

    def shared(label):
        even = flipped(me, label) // 2 * 2
        def rows(p):
            return (even, 2 * p, even, 2 * p + 1, even + 1)
        return rows(parity), rows(1 - parity)

    def step(n, pair, queue):
        amps_of(pair[0], n)
        if len(queue) == LAG:
            gather_both(queue[0], n - LAG)
            queue = queue[1:]
        return queue + (pair,)

    def run(n, pair, queue):
        if not (isinstance(n, int) and n == 0):
            give(n - 1).start()
        if len(queue) == LAG:
            taken(n - LAG)
        return step(n, pair, queue)

    @pl.loop(0, chunks)
    def _(q):
        arrived(1, q)

    turn_all(0)
    turn_all(1)
    queue = run(0, shared(0), ())

    def near_event(t):
        for k in (0, 1):
            q = 2 * t + k
            arrived(2, q)
            arrived(4, q)
            next_sends(q + DEPTH)
            sib_send(q, 2).start()
            sib_send(q, 4).start()
        turn(2, 4, t)
        for k in (0, 1):
            arrived(3, 2 * t + k)
            arrived(5, 2 * t + k)
        turn(3, 5, t)

    def near_pair(c, t):
        return crossed(2 + 3 * c, t - c, 3 + 2 * c, t, 0)

    def near(t, carry):
        near_event(t)
        return lax.fori_loop(
            0, 1 + t % 2, lambda c, g: (g[0] + 1, run(g[0], near_pair(c, t), g[1])), carry
        )

    near_event(0)
    queue = run(1, near_pair(0, 0), queue)
    near_event(1)
    queue = run(2, near_pair(0, 1), queue)
    carry = (jnp.int32(LAG), queue)
    carry = (carry[0] + 1, run(carry[0], near_pair(1, 1), carry[1]))
    carry = lax.fori_loop(2, steps, near, carry)

    def side(m, carry):
        n, queue = carry
        u, t, v = entry(SIDE, 0, m), entry(SIDE, 1, m), entry(SIDE, 2, m)
        return n + 1, run(n, crossed(u, t, u, t + 1, v), queue)

    def own_side(m, carry):
        n, queue = carry
        return n + 1, run(n, shared(2 + 2 * m), queue)

    def far_event(t):
        for k in (0, 1):
            q = 2 * t + k
            arrived(6, q)
            sib_send(q, 6).start()

        @pl.when(chunks + t + DEPTH < chunks + chunks // 2)
        def _():
            next_sends(chunks + t + DEPTH)

    def far_rest(t):
        turn(6, 6, t)
        for k in (0, 1):
            arrived(7, 2 * t + k)
        turn(7, 7, t)

    def far_pair(c, t):
        odd = c // 2
        return crossed(6, t - odd, 7 - odd, t, 4 * (c % 2) + 3 * odd)

    def far(t, carry):
        far_event(t)
        carry = lax.fori_loop(0, (t + 1) % 2 + t % 2, lambda m, g: side(t, g), carry)
        far_rest(t)
        return lax.fori_loop(
            0, 2 + t % 2, lambda c, g: (g[0] + 1, run(g[0], far_pair(c, t), g[1])), carry
        )

    carry = lax.fori_loop(0, 2, own_side, carry)
    carry = lax.fori_loop(0, steps, far, carry)
    n, queue = carry
    queue = run(n, shared(6), queue)
    give(n).start()
    for k in range(LAG):
        taken(n + 1 - LAG + k)
        gather_both(queue[k], n + 1 - LAG + k)

    for u in range(count):
        for c in range(virtuals // LANES):
            wide[c, pl.ds(u, width, count), :] = total[u, :, c * LANES:(c + 1) * LANES]
    for c in range(virtuals // LANES):
        out_ref[:, c * LANES:(c + 1) * LANES] = wide[c].astype(jnp.bfloat16)

    @pl.loop(0, held_a.shape[0])
    def _(n):
        give(n).wait_send()

    @pl.loop(0, steps)
    def _(t):
        for k in (0, 1):
            q = 2 * t + k
            own_send(q, 0).wait_send()
            own_send(q, 1).wait_send()
            for label in (0, 2, 4, 6):
                sib_send(q, label).wait_send()
            far_send(q, 2 if k == 0 else 4).wait_send()


def gathered(factors, occ_energy, vir_energy, coeffs):
    _, virtuals, depth = factors.shape
    count = lax.axis_size("occ")
    width = depth // count
    window = max(
        -(-(d * width % LANES + width) // LANES) * LANES for d in range(count)
    )
    chunks = virtuals // CHUNK
    rounds = count * OFFSETS
    pair_flops = 2 * virtuals * virtuals * (depth + 2 * width)
    gamma = pl.pallas_call(
        gathered_kernel,
        out_shape=jax.ShapeDtypeStruct((count * width, virtuals), jnp.bfloat16),
        in_specs=[pl.BlockSpec(memory_space=pltpu.HBM)] * 3,
        out_specs=pl.BlockSpec(memory_space=pltpu.VMEM),
        scratch_shapes=[
            pltpu.VMEM((count, virtuals, depth), jnp.bfloat16),
            pltpu.VMEM((count, width, virtuals), jnp.bfloat16),
            pltpu.VMEM((count, width, virtuals), jnp.float32),
            pltpu.VMEM((virtuals // LANES, count * width, LANES), jnp.float32),
            pltpu.VMEM((width, window), jnp.bfloat16),
            pltpu.VMEM((virtuals, ROWS), jnp.float32),
            pltpu.VMEM((rounds, virtuals, 2 * ROWS), jnp.bfloat16),
            pltpu.VMEM((rounds, virtuals, 2 * ROWS), jnp.bfloat16),
            pltpu.SMEM((count,), jnp.float32),
            pltpu.VMEM((1, virtuals), jnp.float32),
            pltpu.SemaphoreType.DMA((chunks,)),
            pltpu.SemaphoreType.DMA((2,)),
            pltpu.SemaphoreType.DMA((2, chunks)),
            pltpu.SemaphoreType.DMA((chunks,)),
            pltpu.SemaphoreType.DMA((4, chunks)),
            pltpu.SemaphoreType.DMA((8, chunks)),
            pltpu.SemaphoreType.DMA((rounds,)),
            pltpu.SemaphoreType.DMA((rounds,)),
        ],
        compiler_params=pltpu.CompilerParams(
            collective_id=0, has_side_effects=True, vmem_limit_bytes=52 * 1024 * 1024
        ),
        cost_estimate=pl.CostEstimate(
            flops=count * OFFSETS * pair_flops, bytes_accessed=count * virtuals * depth * 2,
            transcendentals=0,
        ),
    )(factors[0], occ_energy, vir_energy[None])
    back = jnp.dot(gamma, coeffs.T, preferred_element_type=jnp.float32).astype(jnp.bfloat16)
    return back.reshape(width, count, coeffs.shape[0])


def fits(count, virtuals, depth):
    width = depth // count
    return (
        count == 8
        and count == 2 * OFFSETS + 2
        and virtuals == 4 * ROWS
        and depth % (LANES * 2) == 0
        and width % 32 == 0
    )


def either(factors, occ_energy, vir_energy, coeffs):
    if fits(lax.axis_size("occ"), factors.shape[1], factors.shape[2]):
        return gathered(factors, occ_energy, vir_energy, coeffs)
    return on_device(factors, occ_energy, vir_energy, coeffs)


def solution(mesh):
    return jax.shard_map(
        either,
        mesh=mesh,
        in_specs=(P(("frag", "occ"), None, None), P("frag"), P("frag"), P("frag", None)),
        out_specs=P("occ", "frag", None),
        check_vma=False,
    )
```

```python
import jax
import jax.numpy as jnp
from jax import lax
from jax.experimental import pallas as pl
from jax.experimental.pallas import tpu as pltpu
from jax.sharding import PartitionSpec as P

OFFSETS = 3


def passed_along(block, axis, distance):
    devices = range(lax.axis_size(axis))
    route = [((i - distance) % len(devices), i) for i in devices]
    return lax.ppermute(block, axis, route)


def on_device(factors, occ_energy, vir_energy, coeffs):
    mine = factors[0]
    count = lax.axis_size("occ")
    index = lax.axis_index("occ")
    partners = []
    current = mine
    for offset in range(1, OFFSETS + 1):
        current = passed_along(current, "occ", -1)
        partners.append(current)
    own_energy = lax.dynamic_index_in_dim(occ_energy, index, 0, False)
    own = jnp.zeros((mine.shape[1], mine.shape[0]), jnp.float32)
    outgoing = []
    for offset in range(1, OFFSETS + 1):
        partner = partners[offset - 1]
        other_energy = lax.dynamic_index_in_dim(occ_energy, (index + offset) % count, 0, False)
        kmat = lax.dot_general(
            mine, partner, (((1,), (1,)), ((), ())), preferred_element_type=jnp.float32
        )
        denom = own_energy + other_energy - vir_energy[:, None] - vir_energy[None, :]
        amps = (kmat / denom).astype(jnp.bfloat16)
        own = own + lax.dot_general(
            partner, amps, (((0,), (1,)), ((), ())), preferred_element_type=jnp.float32
        )
        sent = lax.dot_general(
            mine, amps, (((0,), (0,)), ((), ())), preferred_element_type=jnp.float32
        )
        outgoing.append(sent.astype(jnp.bfloat16))
    incoming = jnp.zeros_like(own)
    for offset in range(1, OFFSETS + 1):
        arrived = passed_along(outgoing[offset - 1], "occ", offset)
        incoming = incoming + arrived.astype(jnp.float32)
    gamma = (own + incoming).astype(jnp.bfloat16)[None]
    slabs = lax.all_to_all(gamma, "occ", split_axis=1, concat_axis=0, tiled=True)
    return jnp.einsum("ipa,ma->pim", slabs, coeffs, preferred_element_type=jnp.float32).astype(
        jnp.bfloat16
    )


LANES = 128
ROWS = 128
CHUNK = ROWS // 2

BACK_STEPS = 2
DEPTH = 3
AHEAD = 1

ITEMS = (
    ((0, 0, 0, 1, 1, 1), (2, 0, 3, 0, 0, 0)),
    ((2, 1, 3, 1, 0, 0), (5, 0, 5, 1, 0, 0)),
    ((2, 2, 3, 2, 0, 0), (2, 3, 3, 3, 0, 0)),
    ((5, 2, 5, 3, 0, 0), (2, 0, 2, 1, 3, 1)),
    ((4, 0, 4, 1, 5, 1), (2, 0, 2, 1, 4, 0)),
    ((6, 0, 7, 0, 0, 0), (6, 0, 7, 0, 4, 0)),
    ((2, 2, 2, 3, 4, 0), (2, 0, 2, 1, 5, 0)),
    ((6, 1, 7, 1, 0, 0), (6, 1, 7, 1, 4, 0)),
    ((6, 0, 6, 1, 3, 0), (2, 2, 2, 3, 5, 0)),
    ((6, 2, 7, 2, 0, 0), (6, 2, 7, 2, 4, 0)),
    ((6, 3, 7, 3, 0, 0), (6, 3, 7, 3, 4, 0)),
    ((6, 2, 6, 3, 3, 0), (6, 0, 6, 1, 7, 1)),
)
PASSED = (3, 5, 7, 9)
FAR = (5, 7, 9, 10)


def flipped(a, b):
    bits = [(a // w % 2 + b // w % 2) % 2 * w for w in (1, 2, 4)]
    return bits[0] + bits[1] + bits[2]


def octal(packed, n):
    return lax.shift_right_logical(packed, jnp.int32(3) * n) % 8


def pack(ua, ta, ub, tb, v):
    return ua + 8 * ta + 64 * ub + 512 * tb + 4096 * v


def unpack(code):
    return tuple(octal(code, k) for k in range(5))


def gathered_kernel(
    mine_ref, energy_hbm, vir_hbm, out_ref,
    blocks, slabs, total, wide, pick, vcol, held_a, held_b, energy_ref, vir_ref,
    local_sem, small_sem, own_sem, fwd_sem, sib_sem, recv_sem, give_sem, take_sem,
):
    me = lax.axis_index("occ")
    parity = me % 2
    count = blocks.shape[0]
    virtuals, depth = mine_ref.shape
    width = total.shape[1]
    window = pick.shape[1]
    steps = virtuals // ROWS
    chunks = virtuals // CHUNK
    half = virtuals // 2
    rounds = len(ITEMS)
    first = me * width
    lead = pl.multiple_of(first // LANES * LANES, LANES)
    skip = first % LANES

    def rows_of(q):
        return pl.ds(pl.multiple_of(q * CHUNK, CHUNK), CHUNK)

    def local(q):
        return pltpu.make_async_copy(
            mine_ref.at[rows_of(q)], blocks.at[me, rows_of(q)], local_sem.at[q]
        )

    energy_copy = pltpu.make_async_copy(energy_hbm, energy_ref, small_sem.at[0])
    vir_copy = pltpu.make_async_copy(vir_hbm, vir_ref, small_sem.at[1])

    barrier = pltpu.get_barrier_semaphore()
    for bit in (1, 2, 4):
        pl.semaphore_signal(
            barrier, inc=1, device_id={"occ": flipped(me, bit)},
            device_id_type=pl.DeviceIdType.MESH,
        )

    @pl.loop(0, chunks)
    def _(q):
        local(q).start()

    energy_copy.start()
    vir_copy.start()
    pl.semaphore_wait(barrier, 3)

    def send(label, q, bit, send_sem):
        place = blocks.at[flipped(me, label), rows_of(q)]
        return pltpu.make_async_remote_copy(
            src_ref=place,
            dst_ref=place,
            send_sem=send_sem,
            recv_sem=recv_sem.at[flipped(label, bit), q],
            device_id={"occ": flipped(me, bit)},
            device_id_type=pl.DeviceIdType.MESH,
        )

    def own_send(q, axis):
        return send(0, q, 2 + 2 * axis, own_sem.at[axis, q])

    def far_send(q, label):
        return send(label, q, 6 - label, fwd_sem.at[q])

    def sib_send(q, label):
        return send(label, q, 1, sib_sem.at[label // 2, q])

    def arrived(label, q):
        place = blocks.at[flipped(me, label), rows_of(q)]
        pltpu.make_async_copy(place, place, recv_sem.at[label, q]).wait()

    def give(n):
        return pltpu.make_async_remote_copy(
            src_ref=held_a.at[n + 2 * AHEAD],
            dst_ref=held_b.at[n + 2 * AHEAD],
            send_sem=give_sem.at[n],
            recv_sem=take_sem.at[n],
            device_id={"occ": flipped(me, 1)},
            device_id_type=pl.DeviceIdType.MESH,
        )

    def taken(n):
        place = held_b.at[n + 2 * AHEAD]
        pltpu.make_async_copy(place, place, take_sem.at[n]).wait()

    def next_sends(q):
        @pl.when(q < chunks)
        def _():
            own_send(q, 0).start()
            own_send(q, 1).start()

        @pl.when(q >= chunks)
        def _():
            far_send(2 * (q - chunks), 2).start()
            far_send(2 * (q - chunks) + 1, 4).start()

    for q in range(DEPTH):
        local(q).wait()
        own_send(q, 0).start()
        own_send(q, 1).start()
        sib_send(q, 0).start()

    @pl.loop(DEPTH, chunks)
    def _(q):
        local(q).wait()
        sib_send(q, 0).start()

    energy_copy.wait()
    vir_copy.wait()
    total[...] = jnp.zeros_like(total)
    for n in range(2 * AHEAD):
        held_a[n] = jnp.zeros(held_a.shape[1:], held_a.dtype)
        held_b[n] = jnp.zeros(held_b.shape[1:], held_b.dtype)
    column = lax.broadcasted_iota(jnp.int32, (width, window), 1)
    row = lax.broadcasted_iota(jnp.int32, (width, window), 0)
    pick[...] = jnp.where(column == row + skip, 1.0, 0.0).astype(jnp.bfloat16)
    for t in range(steps):
        part = vir_ref[:, t * ROWS:(t + 1) * ROWS]
        vcol[t * ROWS:(t + 1) * ROWS, :] = jnp.broadcast_to(part, (ROWS, ROWS)).T

    def rows_at(t):
        return pl.ds(pl.multiple_of(t * ROWS, ROWS), ROWS)

    def turn_all(label):
        u = flipped(me, label)
        slabs[u] = lax.dot_general(
            pick[...], blocks[u, :, pl.ds(lead, window)], (((1,), (1,)), ((), ())),
            preferred_element_type=jnp.float32,
        ).astype(jnp.bfloat16)

    def turn(la, lb, t):
        ua, ub = flipped(me, la), flipped(me, lb)
        both = jnp.concatenate(
            [blocks[ua, rows_at(t), pl.ds(lead, window)], blocks[ub, rows_at(t), pl.ds(lead, window)]],
            axis=0,
        )
        moved = lax.dot_general(
            pick[...], both, (((1,), (1,)), ((), ())), preferred_element_type=jnp.float32
        ).astype(jnp.bfloat16)
        slabs[ua, :, rows_at(t)] = moved[:, :ROWS]
        slabs[ub, :, rows_at(t)] = moved[:, ROWS:]

    def amps_of(code, n):
        ua, ta, ub, tb, v = unpack(code)
        some = jnp.concatenate([blocks[ua, rows_at(ta), :], blocks[ub, rows_at(tb), :]], axis=0)
        level = jnp.concatenate(
            [energy_ref[ua] - vir_ref[:, rows_at(ta)], energy_ref[ub] - vir_ref[:, rows_at(tb)]],
            axis=1,
        ) + energy_ref[v]
        for h in range(2):
            rows = slice(h * half, (h + 1) * half)
            kmat = lax.dot_general(
                blocks[v, rows, :], some, (((1,), (1,)), ((), ())),
                preferred_element_type=jnp.float32,
            )
            held_a[n, rows, :] = (kmat / (level - vcol[rows, 0:1])).astype(jnp.bfloat16)

    def gather(code, held):
        ua, ta, ub, tb, v = unpack(code)
        left = jnp.concatenate([slabs[ua, :, rows_at(ta)], slabs[ub, :, rows_at(tb)]], axis=1)
        both = jnp.dot(slabs[v], held[...], preferred_element_type=jnp.float32)
        other = lax.dot_general(
            left, held[...], (((1,), (1,)), ((), ())), preferred_element_type=jnp.float32
        )
        total[ua, :, rows_at(ta)] += both[:, :ROWS]
        total[ub, :, rows_at(tb)] += both[:, ROWS:]
        total[v] += other

    def gather_all(codes, n):
        gather(codes[0], held_a.at[n])
        gather(codes[1], held_b.at[n])
        gather(codes[2], held_a.at[n + 1])
        gather(codes[3], held_b.at[n + 1])

    place_of = jnp.int32(0)
    for label in range(8):
        place_of = place_of + flipped(me, label) * 8 ** label

    def codes_of(j):
        codes = []
        for s in range(2):
            packed = jnp.int32(0)
            for k in range(rounds):
                row = ITEMS[k][s]
                packed = jnp.where(j == k, sum(x << (3 * c) for c, x in enumerate(row)), packed)
            lu, ta, lw, tb, lv, same = (octal(packed, c) for c in range(6))
            turned_by = same * parity
            ua, ub, v = (
                octal(place_of, x) for x in (lu + turned_by, lw + turned_by, lv - turned_by)
            )
            codes.append(pack(ua, ta + 2 * turned_by, ub, tb + 2 * turned_by, v))
            swap = 1 - same
            shift = 2 * same * (1 - 2 * parity)
            codes.append(
                pack(
                    ua + swap * (1 - 2 * (ua % 2)), ta + 2 * turned_by + shift,
                    ub + swap * (1 - 2 * (ub % 2)), tb + 2 * turned_by + shift,
                    v + swap * (1 - 2 * (v % 2)),
                )
            )
        return tuple(codes)

    @pl.loop(0, chunks)
    def _(q):
        arrived(1, q)

    turn_all(0)
    turn_all(1)

    def near_event(t):
        for k in (0, 1):
            q = 2 * t + k
            arrived(2, q)
            arrived(4, q)
            next_sends(q + DEPTH)
            sib_send(q, 2).start()
            sib_send(q, 4).start()
        turn(2, 4, t)
        for k in (0, 1):
            arrived(3, 2 * t + k)
            arrived(5, 2 * t + k)
        turn(3, 5, t)

    def pass_far(t):
        for k in (0, 1):
            q = 2 * t + k
            arrived(6, q)
            sib_send(q, 6).start()

        @pl.when(chunks + t + DEPTH < chunks + chunks // 2)
        def _():
            next_sends(chunks + t + DEPTH)

    def far_event(t):
        for k in (0, 1):
            arrived(7, 2 * t + k)
        turn(6, 7, t)

    def at(table, j, event):
        step = jnp.int32(-1)
        for t, k in enumerate(table):
            step = jnp.where(j == k, t, step)

        @pl.when(step >= 0)
        def _():
            event(step)

    def body(j, carry):
        last, now = carry

        @pl.when(j < 2)
        def _():
            near_event(j)

        @pl.when(j == 2)
        def _():
            near_event(j)
            near_event(j + 1)

        at(FAR, j, far_event)
        amps_of(now[0], 2 * j + 2 * AHEAD)
        amps_of(now[2], 2 * j + 2 * AHEAD + 1)
        give(2 * j).start()
        give(2 * j + 1).start()
        at(PASSED, j, pass_far)

        @pl.when(j >= AHEAD)
        def _():
            taken(2 * j - 2 * AHEAD)
            taken(2 * j - 2 * AHEAD + 1)

        gather_all(last, 2 * j)
        return now, codes_of(j + 1)

    first_codes = codes_of(jnp.int32(0))
    nothing = (first_codes[0],) * 4
    last, _ = lax.fori_loop(0, rounds, body, (nothing, first_codes))
    taken(2 * rounds - 2)
    taken(2 * rounds - 1)
    gather_all(last, 2 * rounds)

    for u in range(count):
        for c in range(virtuals // LANES):
            wide[c, pl.ds(u, width, count), :] = total[u, :, c * LANES:(c + 1) * LANES]
    for c in range(virtuals // LANES):
        out_ref[:, c * LANES:(c + 1) * LANES] = wide[c].astype(jnp.bfloat16)

    @pl.loop(0, 2 * rounds)
    def _(n):
        give(n).wait_send()

    @pl.loop(0, steps)
    def _(t):
        for k in (0, 1):
            q = 2 * t + k
            own_send(q, 0).wait_send()
            own_send(q, 1).wait_send()
            for label in (0, 2, 4, 6):
                sib_send(q, label).wait_send()
            far_send(q, 2 if k == 0 else 4).wait_send()


def back_kernel(gamma_ref, coeffs_ref, out_ref):
    out_ref[...] = lax.dot_general(
        gamma_ref[...], coeffs_ref[...], (((1,), (1,)), ((), ())),
        preferred_element_type=jnp.float32,
    ).astype(out_ref.dtype)


def back_of(gamma, coeffs):
    rows, virtuals = gamma.shape
    atomic = coeffs.shape[0]
    block = atomic // BACK_STEPS
    return pl.pallas_call(
        back_kernel,
        grid=(BACK_STEPS,),
        out_shape=jax.ShapeDtypeStruct((rows, atomic), jnp.bfloat16),
        in_specs=[
            pl.BlockSpec((rows, virtuals), lambda i: (0, 0)),
            pl.BlockSpec((block, virtuals), lambda i: (i, 0)),
        ],
        out_specs=pl.BlockSpec((rows, block), lambda i: (0, i)),
        compiler_params=pltpu.CompilerParams(vmem_limit_bytes=32 * 1024 * 1024),
        cost_estimate=pl.CostEstimate(
            flops=2 * rows * virtuals * atomic, transcendentals=0,
            bytes_accessed=2 * (rows * virtuals + atomic * virtuals + rows * atomic),
        ),
    )(gamma, coeffs)


def gathered(factors, occ_energy, vir_energy, coeffs):
    _, virtuals, depth = factors.shape
    count = lax.axis_size("occ")
    width = depth // count
    window = max(
        -(-(d * width % LANES + width) // LANES) * LANES for d in range(count)
    )
    chunks = virtuals // CHUNK
    rounds = count * OFFSETS
    pair_flops = 2 * virtuals * virtuals * (depth + 2 * width)
    gamma = pl.pallas_call(
        gathered_kernel,
        out_shape=jax.ShapeDtypeStruct((count * width, virtuals), jnp.bfloat16),
        in_specs=[pl.BlockSpec(memory_space=pltpu.HBM)] * 3,
        out_specs=pl.BlockSpec(memory_space=pltpu.VMEM),
        scratch_shapes=[
            pltpu.VMEM((count, virtuals, depth), jnp.bfloat16),
            pltpu.VMEM((count, width, virtuals), jnp.bfloat16),
            pltpu.VMEM((count, width, virtuals), jnp.float32),
            pltpu.VMEM((virtuals // LANES, count * width, LANES), jnp.float32),
            pltpu.VMEM((width, window), jnp.bfloat16),
            pltpu.VMEM((virtuals, ROWS), jnp.float32),
            pltpu.VMEM((rounds + 2 * AHEAD, virtuals, 2 * ROWS), jnp.bfloat16),
            pltpu.VMEM((rounds + 2 * AHEAD, virtuals, 2 * ROWS), jnp.bfloat16),
            pltpu.SMEM((count,), jnp.float32),
            pltpu.VMEM((1, virtuals), jnp.float32),
            pltpu.SemaphoreType.DMA((chunks,)),
            pltpu.SemaphoreType.DMA((2,)),
            pltpu.SemaphoreType.DMA((2, chunks)),
            pltpu.SemaphoreType.DMA((chunks,)),
            pltpu.SemaphoreType.DMA((4, chunks)),
            pltpu.SemaphoreType.DMA((8, chunks)),
            pltpu.SemaphoreType.DMA((rounds,)),
            pltpu.SemaphoreType.DMA((rounds,)),
        ],
        compiler_params=pltpu.CompilerParams(
            collective_id=0, has_side_effects=True, vmem_limit_bytes=int(52 * 1024 * 1024)
        ),
        cost_estimate=pl.CostEstimate(
            flops=count * OFFSETS * pair_flops, bytes_accessed=count * virtuals * depth * 2,
            transcendentals=0,
        ),
    )(
        factors[0],
        pltpu.with_memory_space_constraint(occ_energy, pltpu.HBM),
        pltpu.with_memory_space_constraint(vir_energy[None], pltpu.HBM),
    )
    back = back_of(gamma, coeffs)
    return back.reshape(width, count, coeffs.shape[0])


def fits(count, virtuals, depth):
    width = depth // count
    return (
        count == 8
        and count * OFFSETS == 2 * len(ITEMS)
        and virtuals == 4 * ROWS
        and depth % (LANES * 2) == 0
        and width % 32 == 0
    )


def either(factors, occ_energy, vir_energy, coeffs):
    if fits(lax.axis_size("occ"), factors.shape[1], factors.shape[2]):
        return gathered(factors, occ_energy, vir_energy, coeffs)
    return on_device(factors, occ_energy, vir_energy, coeffs)


def solution(mesh):
    return jax.shard_map(
        either,
        mesh=mesh,
        in_specs=(P(("frag", "occ"), None, None), P("frag"), P("frag"), P("frag", None)),
        out_specs=P("occ", "frag", None),
        check_vma=False,
    )
```

```python
import jax
import jax.numpy as jnp
from jax import lax
from jax.experimental import pallas as pl
from jax.experimental.pallas import tpu as pltpu
from jax.sharding import PartitionSpec as P

OFFSETS = 3


def passed_along(block, axis, distance):
    devices = range(lax.axis_size(axis))
    route = [((i - distance) % len(devices), i) for i in devices]
    return lax.ppermute(block, axis, route)


def on_device(factors, occ_energy, vir_energy, coeffs):
    mine = factors[0]
    count = lax.axis_size("occ")
    index = lax.axis_index("occ")
    partners = []
    current = mine
    for offset in range(1, OFFSETS + 1):
        current = passed_along(current, "occ", -1)
        partners.append(current)
    own_energy = lax.dynamic_index_in_dim(occ_energy, index, 0, False)
    own = jnp.zeros((mine.shape[1], mine.shape[0]), jnp.float32)
    outgoing = []
    for offset in range(1, OFFSETS + 1):
        partner = partners[offset - 1]
        other_energy = lax.dynamic_index_in_dim(occ_energy, (index + offset) % count, 0, False)
        kmat = lax.dot_general(
            mine, partner, (((1,), (1,)), ((), ())), preferred_element_type=jnp.float32
        )
        denom = own_energy + other_energy - vir_energy[:, None] - vir_energy[None, :]
        amps = (kmat / denom).astype(jnp.bfloat16)
        own = own + lax.dot_general(
            partner, amps, (((0,), (1,)), ((), ())), preferred_element_type=jnp.float32
        )
        sent = lax.dot_general(
            mine, amps, (((0,), (0,)), ((), ())), preferred_element_type=jnp.float32
        )
        outgoing.append(sent.astype(jnp.bfloat16))
    incoming = jnp.zeros_like(own)
    for offset in range(1, OFFSETS + 1):
        arrived = passed_along(outgoing[offset - 1], "occ", offset)
        incoming = incoming + arrived.astype(jnp.float32)
    gamma = (own + incoming).astype(jnp.bfloat16)[None]
    slabs = lax.all_to_all(gamma, "occ", split_axis=1, concat_axis=0, tiled=True)
    return jnp.einsum("ipa,ma->pim", slabs, coeffs, preferred_element_type=jnp.float32).astype(
        jnp.bfloat16
    )


LANES = 128
ROWS = 128
CHUNK = ROWS // 2

BACK_STEPS = 4
DEPTH = 3

ITEMS = (
    ((0, 0, 0, 1, 1, 1), (0, 0, 0, 1, 1, 1)),
    ((2, 0, 3, 0, 0, 0), (2, 1, 3, 1, 0, 0)),
    ((5, 0, 5, 1, 0, 0), (2, 2, 3, 2, 0, 0)),
    ((2, 3, 3, 3, 0, 0), (5, 2, 5, 3, 0, 0)),
    ((2, 0, 2, 1, 3, 1), (4, 0, 4, 1, 5, 1)),
    ((2, 0, 2, 1, 4, 0), (2, 2, 2, 3, 4, 0)),
    ((6, 0, 7, 0, 0, 0), (6, 0, 7, 0, 4, 0)),
    ((2, 0, 2, 1, 5, 0), (2, 2, 2, 3, 5, 0)),
    ((6, 1, 7, 1, 0, 0), (6, 1, 7, 1, 4, 0)),
    ((6, 2, 7, 2, 0, 0), (6, 2, 7, 2, 4, 0)),
    ((6, 0, 6, 1, 3, 0), (6, 2, 6, 3, 3, 0)),
    ((6, 3, 7, 3, 0, 0), (6, 3, 7, 3, 4, 0)),
    ((6, 0, 6, 1, 7, 1), (6, 0, 6, 1, 7, 1)),
)
PASSED = (4, 6, 7, 9)
FAR = (6, 8, 9, 11)


def flipped(a, b):
    bits = [(a // w % 2 + b // w % 2) % 2 * w for w in (1, 2, 4)]
    return bits[0] + bits[1] + bits[2]


def octal(packed, n):
    return lax.shift_right_logical(packed, jnp.int32(3) * n) % 8


def pack(ua, ta, ub, tb, v):
    return ua + 8 * ta + 64 * ub + 512 * tb + 4096 * v


def unpack(code):
    return tuple(octal(code, k) for k in range(5))


def gathered_kernel(
    mine_ref, energy_hbm, vir_hbm, out_ref,
    blocks, slabs, total, wide, pick, vcol, held_a, held_b, energy_ref, vir_ref,
    local_sem, small_sem, own_sem, fwd_sem, sib_sem, recv_sem, give_sem, take_sem,
):
    me = lax.axis_index("occ")
    parity = me % 2
    count = blocks.shape[0]
    virtuals, depth = mine_ref.shape
    width = total.shape[1]
    window = pick.shape[1]
    steps = virtuals // ROWS
    chunks = virtuals // CHUNK
    half = virtuals // 2
    rounds = len(ITEMS)
    first = me * width
    lead = pl.multiple_of(first // LANES * LANES, LANES)
    skip = first % LANES

    def rows_of(q):
        return pl.ds(pl.multiple_of(q * CHUNK, CHUNK), CHUNK)

    def local(q):
        return pltpu.make_async_copy(
            mine_ref.at[rows_of(q)], blocks.at[me, rows_of(q)], local_sem.at[q]
        )

    energy_copy = pltpu.make_async_copy(energy_hbm, energy_ref, small_sem.at[0])
    vir_copy = pltpu.make_async_copy(vir_hbm, vir_ref, small_sem.at[1])

    barrier = pltpu.get_barrier_semaphore()
    for bit in (1, 2, 4):
        pl.semaphore_signal(
            barrier, inc=1, device_id={"occ": flipped(me, bit)},
            device_id_type=pl.DeviceIdType.MESH,
        )

    @pl.loop(0, chunks)
    def _(q):
        local(q).start()

    energy_copy.start()
    vir_copy.start()
    pl.semaphore_wait(barrier, 3)

    def send(label, q, bit, send_sem):
        place = blocks.at[flipped(me, label), rows_of(q)]
        return pltpu.make_async_remote_copy(
            src_ref=place,
            dst_ref=place,
            send_sem=send_sem,
            recv_sem=recv_sem.at[flipped(label, bit), q],
            device_id={"occ": flipped(me, bit)},
            device_id_type=pl.DeviceIdType.MESH,
        )

    def own_send(q, axis):
        return send(0, q, 2 + 2 * axis, own_sem.at[axis, q])

    def far_send(q, label):
        return send(label, q, 6 - label, fwd_sem.at[q])

    def sib_send(q, label):
        return send(label, q, 1, sib_sem.at[label // 2, q])

    def arrived(label, q):
        place = blocks.at[flipped(me, label), rows_of(q)]
        pltpu.make_async_copy(place, place, recv_sem.at[label, q]).wait()

    def give(n):
        return pltpu.make_async_remote_copy(
            src_ref=held_a.at[n],
            dst_ref=held_b.at[n],
            send_sem=give_sem.at[n],
            recv_sem=take_sem.at[n],
            device_id={"occ": flipped(me, 1)},
            device_id_type=pl.DeviceIdType.MESH,
        )

    def taken(n):
        place = held_b.at[n]
        pltpu.make_async_copy(place, place, take_sem.at[n]).wait()

    def next_sends(q):
        @pl.when(q < chunks)
        def _():
            own_send(q, 0).start()
            own_send(q, 1).start()

        @pl.when(q >= chunks)
        def _():
            far_send(2 * (q - chunks), 2).start()
            far_send(2 * (q - chunks) + 1, 4).start()

    for q in range(DEPTH):
        local(q).wait()
        own_send(q, 0).start()
        own_send(q, 1).start()
        sib_send(q, 0).start()

    @pl.loop(DEPTH, chunks)
    def _(q):
        local(q).wait()
        sib_send(q, 0).start()

    energy_copy.wait()
    vir_copy.wait()
    total[...] = jnp.zeros_like(total)
    for n in range(3):
        held_a[n] = jnp.zeros(held_a.shape[1:], held_a.dtype)
        held_b[n] = jnp.zeros(held_b.shape[1:], held_b.dtype)
    column = lax.broadcasted_iota(jnp.int32, (width, window), 1)
    row = lax.broadcasted_iota(jnp.int32, (width, window), 0)
    pick[...] = jnp.where(column == row + skip, 1.0, 0.0).astype(jnp.bfloat16)
    for t in range(steps):
        part = vir_ref[:, t * ROWS:(t + 1) * ROWS]
        vcol[t * ROWS:(t + 1) * ROWS, :] = jnp.broadcast_to(part, (ROWS, ROWS)).T

    def rows_at(t):
        return pl.ds(pl.multiple_of(t * ROWS, ROWS), ROWS)

    def turn_all(label):
        u = flipped(me, label)
        slabs[u] = lax.dot_general(
            pick[...], blocks[u, :, pl.ds(lead, window)], (((1,), (1,)), ((), ())),
            preferred_element_type=jnp.float32,
        ).astype(jnp.bfloat16)

    def turn(la, lb, t):
        ua, ub = flipped(me, la), flipped(me, lb)
        both = jnp.concatenate(
            [blocks[ua, rows_at(t), pl.ds(lead, window)], blocks[ub, rows_at(t), pl.ds(lead, window)]],
            axis=0,
        )
        moved = lax.dot_general(
            pick[...], both, (((1,), (1,)), ((), ())), preferred_element_type=jnp.float32
        ).astype(jnp.bfloat16)
        slabs[ua, :, rows_at(t)] = moved[:, :ROWS]
        slabs[ub, :, rows_at(t)] = moved[:, ROWS:]

    def amps_of(code, n):
        ua, ta, ub, tb, v = unpack(code)
        some = jnp.concatenate([blocks[ua, rows_at(ta), :], blocks[ub, rows_at(tb), :]], axis=0)
        level = jnp.concatenate(
            [energy_ref[ua] - vir_ref[:, rows_at(ta)], energy_ref[ub] - vir_ref[:, rows_at(tb)]],
            axis=1,
        ) + energy_ref[v]
        for h in range(2):
            rows = slice(h * half, (h + 1) * half)
            kmat = lax.dot_general(
                blocks[v, rows, :], some, (((1,), (1,)), ((), ())),
                preferred_element_type=jnp.float32,
            )
            held_a[n, rows, :] = (kmat / (level - vcol[rows, 0:1])).astype(jnp.bfloat16)

    def gather(code, held):
        ua, ta, ub, tb, v = unpack(code)
        left = jnp.concatenate([slabs[ua, :, rows_at(ta)], slabs[ub, :, rows_at(tb)]], axis=1)
        both = jnp.dot(slabs[v], held[...], preferred_element_type=jnp.float32)
        other = lax.dot_general(
            left, held[...], (((1,), (1,)), ((), ())), preferred_element_type=jnp.float32
        )
        total[ua, :, rows_at(ta)] += both[:, :ROWS]
        total[ub, :, rows_at(tb)] += both[:, ROWS:]
        total[v] += other

    def gather_all(codes, n):
        gather(codes[0], held_a.at[n])
        gather(codes[1], held_b.at[n])
        gather(codes[2], held_a.at[n + 1])
        gather(codes[3], held_b.at[n + 1])

    place_of = jnp.int32(0)
    for label in range(8):
        place_of = place_of + flipped(me, label) * 8 ** label

    def codes_of(j):
        codes = []
        for s in range(2):
            packed = jnp.int32(0)
            for k in range(rounds):
                row = ITEMS[k][s]
                packed = jnp.where(j == k, sum(x << (3 * c) for c, x in enumerate(row)), packed)
            lu, ta, lw, tb, lv, same = (octal(packed, c) for c in range(6))
            turned_by = same * parity
            ua, ub, v = (
                octal(place_of, x) for x in (lu + turned_by, lw + turned_by, lv - turned_by)
            )
            codes.append(pack(ua, ta + 2 * turned_by, ub, tb + 2 * turned_by, v))
            swap = 1 - same
            shift = 2 * same * (1 - 2 * parity)
            codes.append(
                pack(
                    ua + swap * (1 - 2 * (ua % 2)), ta + 2 * turned_by + shift,
                    ub + swap * (1 - 2 * (ub % 2)), tb + 2 * turned_by + shift,
                    v + swap * (1 - 2 * (v % 2)),
                )
            )
        return tuple(codes)

    @pl.loop(0, chunks)
    def _(q):
        arrived(1, q)

    turn_all(0)
    turn_all(1)

    def near_event(t):
        for k in (0, 1):
            q = 2 * t + k
            arrived(2, q)
            arrived(4, q)
            next_sends(q + DEPTH)
            sib_send(q, 2).start()
            sib_send(q, 4).start()
        turn(2, 4, t)
        for k in (0, 1):
            arrived(3, 2 * t + k)
            arrived(5, 2 * t + k)
        turn(3, 5, t)

    def pass_far(t):
        for k in (0, 1):
            q = 2 * t + k
            arrived(6, q)
            sib_send(q, 6).start()

        @pl.when(chunks + t + DEPTH < chunks + chunks // 2)
        def _():
            next_sends(chunks + t + DEPTH)

    def far_event(t):
        for k in (0, 1):
            arrived(7, 2 * t + k)
        turn(6, 7, t)

    def at(table, j, event):
        step = jnp.int32(-1)
        for t, k in enumerate(table):
            step = jnp.where(j == k, t, step)

        @pl.when(step >= 0)
        def _():
            event(step)

    def body(j, carry):
        last, mid, now = carry

        @pl.when(j == 1)
        def _():
            near_event(0)

        @pl.when(j <= 3)
        def _():
            near_event(j)

        at(FAR, j, far_event)
        amps_of(now[0], 2 * j + 2)
        amps_of(now[2], 2 * j + 3)
        give(2 * j + 2).start()
        give(2 * j + 3).start()
        at(PASSED, j, pass_far)

        @pl.when(j >= 2)
        def _():
            taken(2 * j - 1)

        @pl.when(j >= 3)
        def _():
            taken(2 * j - 2)

        gather_all(last, 2 * j - 2)
        return mid, now, codes_of(j + 1)

    front = codes_of(jnp.int32(0))
    amps_of(front[2], 3)
    give(3).start()
    final = rounds - 1
    last, mid, now = lax.fori_loop(1, final, body, (front, front, codes_of(jnp.int32(1))))
    amps_of(now[0], 2 * final + 2)
    give(2 * final + 2).start()
    taken(2 * final - 2)
    taken(2 * final - 1)
    gather_all(last, 2 * final - 2)
    taken(2 * final)
    taken(2 * final + 1)
    gather_all(mid, 2 * final)
    gather(now[0], held_a.at[2 * final + 2])
    taken(2 * final + 2)
    gather(now[1], held_b.at[2 * final + 2])

    for u in range(count):
        for c in range(virtuals // LANES):
            wide[c, pl.ds(u, width, count), :] = total[u, :, c * LANES:(c + 1) * LANES]
    for c in range(virtuals // LANES):
        out_ref[:, c * LANES:(c + 1) * LANES] = wide[c].astype(jnp.bfloat16)

    @pl.loop(3, 2 * rounds + 1)
    def _(n):
        give(n).wait_send()

    @pl.loop(0, steps)
    def _(t):
        for k in (0, 1):
            q = 2 * t + k
            own_send(q, 0).wait_send()
            own_send(q, 1).wait_send()
            for label in (0, 2, 4, 6):
                sib_send(q, label).wait_send()
            far_send(q, 2 if k == 0 else 4).wait_send()


def back_kernel(gamma_ref, coeffs_ref, out_ref, done, done_sem):
    block = done.shape[1]

    def put(i):
        return pltpu.make_async_copy(
            done.at[i], out_ref.at[pl.ds(i * block, block)], done_sem.at[i]
        )

    for i in range(BACK_STEPS):
        done[i] = lax.dot_general(
            gamma_ref[i * block:(i + 1) * block, :], coeffs_ref[...], (((1,), (1,)), ((), ())),
            preferred_element_type=jnp.float32,
        ).astype(done.dtype)
        put(i).start()
    for i in range(BACK_STEPS):
        put(i).wait()


def back_of(gamma, coeffs):
    rows, virtuals = gamma.shape
    atomic = coeffs.shape[0]
    return pl.pallas_call(
        back_kernel,
        out_shape=jax.ShapeDtypeStruct((rows, atomic), jnp.bfloat16),
        in_specs=[pl.BlockSpec(memory_space=pltpu.VMEM)] * 2,
        out_specs=pl.BlockSpec(memory_space=pltpu.HBM),
        scratch_shapes=[
            pltpu.VMEM((BACK_STEPS, rows // BACK_STEPS, atomic), jnp.bfloat16),
            pltpu.SemaphoreType.DMA((BACK_STEPS,)),
        ],
        compiler_params=pltpu.CompilerParams(vmem_limit_bytes=32 * 1024 * 1024),
        cost_estimate=pl.CostEstimate(
            flops=2 * rows * virtuals * atomic, transcendentals=0,
            bytes_accessed=2 * (rows * virtuals + atomic * virtuals + rows * atomic),
        ),
    )(gamma, coeffs)


def gathered(factors, occ_energy, vir_energy, coeffs):
    _, virtuals, depth = factors.shape
    count = lax.axis_size("occ")
    width = depth // count
    window = max(
        -(-(d * width % LANES + width) // LANES) * LANES for d in range(count)
    )
    chunks = virtuals // CHUNK
    pair_flops = 2 * virtuals * virtuals * (depth + 2 * width)
    gamma = pl.pallas_call(
        gathered_kernel,
        out_shape=jax.ShapeDtypeStruct((count * width, virtuals), jnp.bfloat16),
        in_specs=[pl.BlockSpec(memory_space=pltpu.HBM)] * 3,
        out_specs=pl.BlockSpec(memory_space=pltpu.VMEM),
        scratch_shapes=[
            pltpu.VMEM((count, virtuals, depth), jnp.bfloat16),
            pltpu.VMEM((count, width, virtuals), jnp.bfloat16),
            pltpu.VMEM((count, width, virtuals), jnp.float32),
            pltpu.VMEM((virtuals // LANES, count * width, LANES), jnp.float32),
            pltpu.VMEM((width, window), jnp.bfloat16),
            pltpu.VMEM((virtuals, ROWS), jnp.float32),
            pltpu.VMEM((2 * len(ITEMS) + 1, virtuals, 2 * ROWS), jnp.bfloat16),
            pltpu.VMEM((2 * len(ITEMS) + 1, virtuals, 2 * ROWS), jnp.bfloat16),
            pltpu.SMEM((count,), jnp.float32),
            pltpu.VMEM((1, virtuals), jnp.float32),
            pltpu.SemaphoreType.DMA((chunks,)),
            pltpu.SemaphoreType.DMA((2,)),
            pltpu.SemaphoreType.DMA((2, chunks)),
            pltpu.SemaphoreType.DMA((chunks,)),
            pltpu.SemaphoreType.DMA((4, chunks)),
            pltpu.SemaphoreType.DMA((8, chunks)),
            pltpu.SemaphoreType.DMA((2 * len(ITEMS) + 1,)),
            pltpu.SemaphoreType.DMA((2 * len(ITEMS) + 1,)),
        ],
        compiler_params=pltpu.CompilerParams(
            collective_id=0, has_side_effects=True, vmem_limit_bytes=int(52 * 1024 * 1024)
        ),
        cost_estimate=pl.CostEstimate(
            flops=count * OFFSETS * pair_flops, bytes_accessed=count * virtuals * depth * 2,
            transcendentals=0,
        ),
    )(
        factors[0],
        pltpu.with_memory_space_constraint(occ_energy, pltpu.HBM),
        pltpu.with_memory_space_constraint(vir_energy[None], pltpu.HBM),
    )
    back = back_of(gamma, coeffs)
    return back.reshape(width, count, coeffs.shape[0])


def fits(count, virtuals, depth):
    width = depth // count
    return (
        count == 8
        and count * OFFSETS == 2 * len(ITEMS) - 2
        and virtuals == 4 * ROWS
        and depth % (LANES * 2) == 0
        and width % 32 == 0
    )


def either(factors, occ_energy, vir_energy, coeffs):
    if fits(lax.axis_size("occ"), factors.shape[1], factors.shape[2]):
        return gathered(factors, occ_energy, vir_energy, coeffs)
    return on_device(factors, occ_energy, vir_energy, coeffs)


def solution(mesh):
    return jax.shard_map(
        either,
        mesh=mesh,
        in_specs=(P(("frag", "occ"), None, None), P("frag"), P("frag"), P("frag", None)),
        out_specs=P("occ", "frag", None),
        check_vma=False,
    )
```

```python
import jax
import jax.numpy as jnp
from jax import lax
from jax.experimental import pallas as pl
from jax.experimental.pallas import tpu as pltpu
from jax.sharding import PartitionSpec as P

OFFSETS = 3


def passed_along(block, axis, distance):
    devices = range(lax.axis_size(axis))
    route = [((i - distance) % len(devices), i) for i in devices]
    return lax.ppermute(block, axis, route)


def on_device(factors, occ_energy, vir_energy, coeffs):
    mine = factors[0]
    count = lax.axis_size("occ")
    index = lax.axis_index("occ")
    partners = []
    current = mine
    for offset in range(1, OFFSETS + 1):
        current = passed_along(current, "occ", -1)
        partners.append(current)
    own_energy = lax.dynamic_index_in_dim(occ_energy, index, 0, False)
    own = jnp.zeros((mine.shape[1], mine.shape[0]), jnp.float32)
    outgoing = []
    for offset in range(1, OFFSETS + 1):
        partner = partners[offset - 1]
        other_energy = lax.dynamic_index_in_dim(occ_energy, (index + offset) % count, 0, False)
        kmat = lax.dot_general(
            mine, partner, (((1,), (1,)), ((), ())), preferred_element_type=jnp.float32
        )
        denom = own_energy + other_energy - vir_energy[:, None] - vir_energy[None, :]
        amps = (kmat / denom).astype(jnp.bfloat16)
        own = own + lax.dot_general(
            partner, amps, (((0,), (1,)), ((), ())), preferred_element_type=jnp.float32
        )
        sent = lax.dot_general(
            mine, amps, (((0,), (0,)), ((), ())), preferred_element_type=jnp.float32
        )
        outgoing.append(sent.astype(jnp.bfloat16))
    incoming = jnp.zeros_like(own)
    for offset in range(1, OFFSETS + 1):
        arrived = passed_along(outgoing[offset - 1], "occ", offset)
        incoming = incoming + arrived.astype(jnp.float32)
    gamma = (own + incoming).astype(jnp.bfloat16)[None]
    slabs = lax.all_to_all(gamma, "occ", split_axis=1, concat_axis=0, tiled=True)
    return jnp.einsum("ipa,ma->pim", slabs, coeffs, preferred_element_type=jnp.float32).astype(
        jnp.bfloat16
    )


LANES = 128
ROWS = 128
CHUNK = ROWS // 2

BACK_STEPS = 4
DEPTH = 3

ITEMS = (
    ((0, 0, 0, 1, 1, 1), (0, 0, 0, 1, 1, 1)),
    ((2, 0, 3, 0, 0, 0), (2, 1, 3, 1, 0, 0)),
    ((5, 0, 5, 1, 0, 0), (2, 2, 3, 2, 0, 0)),
    ((2, 0, 2, 1, 4, 0), (2, 2, 2, 3, 4, 0)),
    ((2, 0, 2, 1, 3, 1), (4, 0, 4, 1, 5, 1)),
    ((2, 3, 3, 3, 0, 0), (5, 2, 5, 3, 0, 0)),
    ((6, 0, 7, 0, 0, 0), (6, 0, 7, 0, 4, 0)),
    ((2, 0, 2, 1, 5, 0), (2, 2, 2, 3, 5, 0)),
    ((6, 1, 7, 1, 0, 0), (6, 1, 7, 1, 4, 0)),
    ((6, 2, 7, 2, 0, 0), (6, 2, 7, 2, 4, 0)),
    ((6, 0, 6, 1, 3, 0), (6, 2, 6, 3, 3, 0)),
    ((6, 3, 7, 3, 0, 0), (6, 3, 7, 3, 4, 0)),
    ((6, 0, 6, 1, 7, 1), (6, 0, 6, 1, 7, 1)),
)
PASSED = (4, 6, 8, 9)
FAR = (6, 8, 9, 11)


def flipped(a, b):
    bits = [(a // w % 2 + b // w % 2) % 2 * w for w in (1, 2, 4)]
    return bits[0] + bits[1] + bits[2]


def octal(packed, n):
    return lax.shift_right_logical(packed, jnp.int32(3) * n) % 8


def pack(ua, ta, ub, tb, v):
    return ua + 8 * ta + 64 * ub + 512 * tb + 4096 * v


def unpack(code):
    return tuple(octal(code, k) for k in range(5))


def gathered_kernel(
    mine_ref, energy_hbm, vir_hbm, out_ref,
    blocks, slabs, total, wide, pick, vcol, held_a, held_b, energy_ref, vir_ref,
    local_sem, small_sem, own_sem, fwd_sem, sib_sem, recv_sem, give_sem, take_sem,
):
    me = lax.axis_index("occ")
    parity = me % 2
    count = blocks.shape[0]
    virtuals, depth = mine_ref.shape
    width = total.shape[1]
    window = pick.shape[1]
    steps = virtuals // ROWS
    chunks = virtuals // CHUNK
    half = virtuals // 2
    rounds = len(ITEMS)
    first = me * width
    lead = pl.multiple_of(first // LANES * LANES, LANES)
    skip = first % LANES

    def rows_of(q):
        return pl.ds(pl.multiple_of(q * CHUNK, CHUNK), CHUNK)

    def local(q):
        return pltpu.make_async_copy(
            mine_ref.at[rows_of(q)], blocks.at[me, rows_of(q)], local_sem.at[q]
        )

    energy_copy = pltpu.make_async_copy(energy_hbm, energy_ref, small_sem.at[0])
    vir_copy = pltpu.make_async_copy(vir_hbm, vir_ref, small_sem.at[1])

    barrier = pltpu.get_barrier_semaphore()
    for bit in (1, 2, 4):
        pl.semaphore_signal(
            barrier, inc=1, device_id={"occ": flipped(me, bit)},
            device_id_type=pl.DeviceIdType.MESH,
        )

    @pl.loop(0, chunks)
    def _(q):
        local(q).start()

    energy_copy.start()
    vir_copy.start()
    pl.semaphore_wait(barrier, 3)

    def send(label, q, bit, send_sem):
        place = blocks.at[flipped(me, label), rows_of(q)]
        return pltpu.make_async_remote_copy(
            src_ref=place,
            dst_ref=place,
            send_sem=send_sem,
            recv_sem=recv_sem.at[flipped(label, bit), q],
            device_id={"occ": flipped(me, bit)},
            device_id_type=pl.DeviceIdType.MESH,
        )

    def own_send(q, axis):
        return send(0, q, 2 + 2 * axis, own_sem.at[axis, q])

    def far_send(q, label):
        return send(label, q, 6 - label, fwd_sem.at[q])

    def sib_send(q, label):
        return send(label, q, 1, sib_sem.at[label // 2, q])

    def arrived(label, q):
        place = blocks.at[flipped(me, label), rows_of(q)]
        pltpu.make_async_copy(place, place, recv_sem.at[label, q]).wait()

    def give(n):
        return pltpu.make_async_remote_copy(
            src_ref=held_a.at[n],
            dst_ref=held_b.at[n],
            send_sem=give_sem.at[n],
            recv_sem=take_sem.at[n],
            device_id={"occ": flipped(me, 1)},
            device_id_type=pl.DeviceIdType.MESH,
        )

    def taken(n):
        place = held_b.at[n]
        pltpu.make_async_copy(place, place, take_sem.at[n]).wait()

    def next_sends(q):
        @pl.when(q < chunks)
        def _():
            own_send(q, 0).start()
            own_send(q, 1).start()

        @pl.when(q >= chunks)
        def _():
            far_send(2 * (q - chunks), 2).start()
            far_send(2 * (q - chunks) + 1, 4).start()

    for q in range(DEPTH):
        local(q).wait()
        own_send(q, 0).start()
        own_send(q, 1).start()
        sib_send(q, 0).start()

    @pl.loop(DEPTH, chunks)
    def _(q):
        local(q).wait()
        sib_send(q, 0).start()

    energy_copy.wait()
    vir_copy.wait()
    total[...] = jnp.zeros_like(total)
    for n in range(3):
        held_a[n] = jnp.zeros(held_a.shape[1:], held_a.dtype)
        held_b[n] = jnp.zeros(held_b.shape[1:], held_b.dtype)
    column = lax.broadcasted_iota(jnp.int32, (width, window), 1)
    row = lax.broadcasted_iota(jnp.int32, (width, window), 0)
    pick[...] = jnp.where(column == row + skip, 1.0, 0.0).astype(jnp.bfloat16)
    for t in range(steps):
        part = vir_ref[:, t * ROWS:(t + 1) * ROWS]
        vcol[t * ROWS:(t + 1) * ROWS, :] = jnp.broadcast_to(part, (ROWS, ROWS)).T

    def rows_at(t):
        return pl.ds(pl.multiple_of(t * ROWS, ROWS), ROWS)

    def turn_all(label):
        u = flipped(me, label)
        slabs[u] = lax.dot_general(
            pick[...], blocks[u, :, pl.ds(lead, window)], (((1,), (1,)), ((), ())),
            preferred_element_type=jnp.float32,
        ).astype(jnp.bfloat16)

    def turn(la, lb, t):
        ua, ub = flipped(me, la), flipped(me, lb)
        both = jnp.concatenate(
            [blocks[ua, rows_at(t), pl.ds(lead, window)], blocks[ub, rows_at(t), pl.ds(lead, window)]],
            axis=0,
        )
        moved = lax.dot_general(
            pick[...], both, (((1,), (1,)), ((), ())), preferred_element_type=jnp.float32
        ).astype(jnp.bfloat16)
        slabs[ua, :, rows_at(t)] = moved[:, :ROWS]
        slabs[ub, :, rows_at(t)] = moved[:, ROWS:]

    def amps_of(code, n):
        ua, ta, ub, tb, v = unpack(code)
        some = jnp.concatenate([blocks[ua, rows_at(ta), :], blocks[ub, rows_at(tb), :]], axis=0)
        level = jnp.concatenate(
            [energy_ref[ua] - vir_ref[:, rows_at(ta)], energy_ref[ub] - vir_ref[:, rows_at(tb)]],
            axis=1,
        ) + energy_ref[v]
        for h in range(2):
            rows = slice(h * half, (h + 1) * half)
            kmat = lax.dot_general(
                blocks[v, rows, :], some, (((1,), (1,)), ((), ())),
                preferred_element_type=jnp.float32,
            )
            held_a[n, rows, :] = (kmat / (level - vcol[rows, 0:1])).astype(jnp.bfloat16)

    def gather(code, held):
        ua, ta, ub, tb, v = unpack(code)
        left = jnp.concatenate([slabs[ua, :, rows_at(ta)], slabs[ub, :, rows_at(tb)]], axis=1)
        both = jnp.dot(slabs[v], held[...], preferred_element_type=jnp.float32)
        other = lax.dot_general(
            left, held[...], (((1,), (1,)), ((), ())), preferred_element_type=jnp.float32
        )
        total[ua, :, rows_at(ta)] += both[:, :ROWS]
        total[ub, :, rows_at(tb)] += both[:, ROWS:]
        total[v] += other

    def gather_all(codes, n):
        gather(codes[0], held_a.at[n])
        gather(codes[1], held_b.at[n])
        gather(codes[2], held_a.at[n + 1])
        gather(codes[3], held_b.at[n + 1])

    place_of = jnp.int32(0)
    for label in range(8):
        place_of = place_of + flipped(me, label) * 8 ** label

    def codes_of(j):
        codes = []
        for s in range(2):
            packed = jnp.int32(0)
            for k in range(rounds):
                row = ITEMS[k][s]
                packed = jnp.where(j == k, sum(x << (3 * c) for c, x in enumerate(row)), packed)
            lu, ta, lw, tb, lv, same = (octal(packed, c) for c in range(6))
            turned_by = same * parity
            ua, ub, v = (
                octal(place_of, x) for x in (lu + turned_by, lw + turned_by, lv - turned_by)
            )
            codes.append(pack(ua, ta + 2 * turned_by, ub, tb + 2 * turned_by, v))
            swap = 1 - same
            shift = 2 * same * (1 - 2 * parity)
            codes.append(
                pack(
                    ua + swap * (1 - 2 * (ua % 2)), ta + 2 * turned_by + shift,
                    ub + swap * (1 - 2 * (ub % 2)), tb + 2 * turned_by + shift,
                    v + swap * (1 - 2 * (v % 2)),
                )
            )
        return tuple(codes)

    @pl.loop(0, chunks)
    def _(q):
        arrived(1, q)

    turn_all(0)
    turn_all(1)

    def near_pass(t):
        for k in (0, 1):
            q = 2 * t + k
            arrived(2, q)
            arrived(4, q)
            next_sends(q + DEPTH)
            sib_send(q, 2).start()
            sib_send(q, 4).start()

    def near_take(t):
        turn(2, 4, t)
        for k in (0, 1):
            arrived(3, 2 * t + k)
            arrived(5, 2 * t + k)
        turn(3, 5, t)

    def pass_far(t):
        for k in (0, 1):
            q = 2 * t + k
            arrived(6, q)
            sib_send(q, 6).start()

        @pl.when(chunks + t + DEPTH < chunks + chunks // 2)
        def _():
            next_sends(chunks + t + DEPTH)

    def far_event(t):
        for k in (0, 1):
            arrived(7, 2 * t + k)
        turn(6, 7, t)

    def at(table, j, event):
        step = jnp.int32(-1)
        for t, k in enumerate(table):
            step = jnp.where(j == k, t, step)

        @pl.when(step >= 0)
        def _():
            event(step)

    def body(j, carry):
        last, mid, now = carry

        @pl.when(j == 1)
        def _():
            near_pass(0)
            near_take(0)

        @pl.when(j <= steps - 1)
        def _():
            near_pass(j)

        @pl.when((j <= steps - 2) | (j == steps))
        def _():
            near_take(j - j // steps)

        at(FAR, j, far_event)
        amps_of(now[0], 2 * j + 2)
        amps_of(now[2], 2 * j + 3)
        give(2 * j + 2).start()
        give(2 * j + 3).start()
        at(PASSED, j, pass_far)

        @pl.when(j >= 2)
        def _():
            taken(2 * j - 1)

        @pl.when(j >= 3)
        def _():
            taken(2 * j - 2)

        gather_all(last, 2 * j - 2)
        return mid, now, codes_of(j + 1)

    front = codes_of(jnp.int32(0))
    amps_of(front[2], 3)
    give(3).start()
    final = rounds - 1
    last, mid, now = lax.fori_loop(1, final, body, (front, front, codes_of(jnp.int32(1))))
    amps_of(now[0], 2 * final + 2)
    give(2 * final + 2).start()
    taken(2 * final - 2)
    taken(2 * final - 1)
    gather_all(last, 2 * final - 2)
    taken(2 * final)
    taken(2 * final + 1)
    gather_all(mid, 2 * final)
    gather(now[0], held_a.at[2 * final + 2])

    def spread(label):
        u = flipped(me, label)
        for c in range(virtuals // LANES):
            wide[c, pl.ds(u, width, count), :] = total[u, :, c * LANES:(c + 1) * LANES]

    for label in range(6):
        spread(label)
    taken(2 * final + 2)
    gather(now[1], held_b.at[2 * final + 2])
    for label in (6, 7):
        spread(label)
    for c in range(virtuals // LANES):
        out_ref[:, c * LANES:(c + 1) * LANES] = wide[c].astype(jnp.bfloat16)

    @pl.loop(3, 2 * rounds + 1)
    def _(n):
        give(n).wait_send()

    @pl.loop(0, steps)
    def _(t):
        for k in (0, 1):
            q = 2 * t + k
            own_send(q, 0).wait_send()
            own_send(q, 1).wait_send()
            for label in (0, 2, 4, 6):
                sib_send(q, label).wait_send()
            far_send(q, 2 if k == 0 else 4).wait_send()


def back_kernel(gamma_ref, coeffs_ref, out_ref, done, done_sem):
    block = done.shape[1]

    def put(i):
        return pltpu.make_async_copy(
            done.at[i], out_ref.at[pl.ds(i * block, block)], done_sem.at[i]
        )

    for i in range(BACK_STEPS):
        done[i] = lax.dot_general(
            gamma_ref[i * block:(i + 1) * block, :], coeffs_ref[...], (((1,), (1,)), ((), ())),
            preferred_element_type=jnp.float32,
        ).astype(done.dtype)
        put(i).start()
    for i in range(BACK_STEPS):
        put(i).wait()


def back_of(gamma, coeffs):
    rows, virtuals = gamma.shape
    atomic = coeffs.shape[0]
    return pl.pallas_call(
        back_kernel,
        out_shape=jax.ShapeDtypeStruct((rows, atomic), jnp.bfloat16),
        in_specs=[pl.BlockSpec(memory_space=pltpu.VMEM)] * 2,
        out_specs=pl.BlockSpec(memory_space=pltpu.HBM),
        scratch_shapes=[
            pltpu.VMEM((BACK_STEPS, rows // BACK_STEPS, atomic), jnp.bfloat16),
            pltpu.SemaphoreType.DMA((BACK_STEPS,)),
        ],
        compiler_params=pltpu.CompilerParams(vmem_limit_bytes=32 * 1024 * 1024),
        cost_estimate=pl.CostEstimate(
            flops=2 * rows * virtuals * atomic, transcendentals=0,
            bytes_accessed=2 * (rows * virtuals + atomic * virtuals + rows * atomic),
        ),
    )(gamma, coeffs)


def gathered(factors, occ_energy, vir_energy, coeffs):
    _, virtuals, depth = factors.shape
    count = lax.axis_size("occ")
    width = depth // count
    window = max(
        -(-(d * width % LANES + width) // LANES) * LANES for d in range(count)
    )
    chunks = virtuals // CHUNK
    pair_flops = 2 * virtuals * virtuals * (depth + 2 * width)
    gamma = pl.pallas_call(
        gathered_kernel,
        out_shape=jax.ShapeDtypeStruct((count * width, virtuals), jnp.bfloat16),
        in_specs=[pl.BlockSpec(memory_space=pltpu.HBM)] * 3,
        out_specs=pl.BlockSpec(memory_space=pltpu.VMEM),
        scratch_shapes=[
            pltpu.VMEM((count, virtuals, depth), jnp.bfloat16),
            pltpu.VMEM((count, width, virtuals), jnp.bfloat16),
            pltpu.VMEM((count, width, virtuals), jnp.float32),
            pltpu.VMEM((virtuals // LANES, count * width, LANES), jnp.float32),
            pltpu.VMEM((width, window), jnp.bfloat16),
            pltpu.VMEM((virtuals, ROWS), jnp.float32),
            pltpu.VMEM((2 * len(ITEMS) + 1, virtuals, 2 * ROWS), jnp.bfloat16),
            pltpu.VMEM((2 * len(ITEMS) + 1, virtuals, 2 * ROWS), jnp.bfloat16),
            pltpu.SMEM((count,), jnp.float32),
            pltpu.VMEM((1, virtuals), jnp.float32),
            pltpu.SemaphoreType.DMA((chunks,)),
            pltpu.SemaphoreType.DMA((2,)),
            pltpu.SemaphoreType.DMA((2, chunks)),
            pltpu.SemaphoreType.DMA((chunks,)),
            pltpu.SemaphoreType.DMA((4, chunks)),
            pltpu.SemaphoreType.DMA((8, chunks)),
            pltpu.SemaphoreType.DMA((2 * len(ITEMS) + 1,)),
            pltpu.SemaphoreType.DMA((2 * len(ITEMS) + 1,)),
        ],
        compiler_params=pltpu.CompilerParams(
            collective_id=0, has_side_effects=True, vmem_limit_bytes=int(52 * 1024 * 1024)
        ),
        cost_estimate=pl.CostEstimate(
            flops=count * OFFSETS * pair_flops, bytes_accessed=count * virtuals * depth * 2,
            transcendentals=0,
        ),
    )(
        factors[0],
        pltpu.with_memory_space_constraint(occ_energy, pltpu.HBM),
        pltpu.with_memory_space_constraint(vir_energy[None], pltpu.HBM),
    )
    back = back_of(gamma, coeffs)
    return back.reshape(width, count, coeffs.shape[0])


def fits(count, virtuals, depth):
    width = depth // count
    return (
        count == 8
        and count * OFFSETS == 2 * len(ITEMS) - 2
        and virtuals == 4 * ROWS
        and depth % (LANES * 2) == 0
        and width % 32 == 0
    )


def either(factors, occ_energy, vir_energy, coeffs):
    if fits(lax.axis_size("occ"), factors.shape[1], factors.shape[2]):
        return gathered(factors, occ_energy, vir_energy, coeffs)
    return on_device(factors, occ_energy, vir_energy, coeffs)


def solution(mesh):
    return jax.shard_map(
        either,
        mesh=mesh,
        in_specs=(P(("frag", "occ"), None, None), P("frag"), P("frag"), P("frag", None)),
        out_specs=P("occ", "frag", None),
        check_vma=False,
    )
```

```python
import jax
import jax.numpy as jnp
from jax import lax
from jax.experimental import pallas as pl
from jax.experimental.pallas import tpu as pltpu
from jax.sharding import PartitionSpec as P

OFFSETS = 3


def passed_along(block, axis, distance):
    devices = range(lax.axis_size(axis))
    route = [((i - distance) % len(devices), i) for i in devices]
    return lax.ppermute(block, axis, route)


def on_device(factors, occ_energy, vir_energy, coeffs):
    mine = factors[0]
    count = lax.axis_size("occ")
    index = lax.axis_index("occ")
    partners = []
    current = mine
    for offset in range(1, OFFSETS + 1):
        current = passed_along(current, "occ", -1)
        partners.append(current)
    own_energy = lax.dynamic_index_in_dim(occ_energy, index, 0, False)
    own = jnp.zeros((mine.shape[1], mine.shape[0]), jnp.float32)
    outgoing = []
    for offset in range(1, OFFSETS + 1):
        partner = partners[offset - 1]
        other_energy = lax.dynamic_index_in_dim(occ_energy, (index + offset) % count, 0, False)
        kmat = lax.dot_general(
            mine, partner, (((1,), (1,)), ((), ())), preferred_element_type=jnp.float32
        )
        denom = own_energy + other_energy - vir_energy[:, None] - vir_energy[None, :]
        amps = (kmat / denom).astype(jnp.bfloat16)
        own = own + lax.dot_general(
            partner, amps, (((0,), (1,)), ((), ())), preferred_element_type=jnp.float32
        )
        sent = lax.dot_general(
            mine, amps, (((0,), (0,)), ((), ())), preferred_element_type=jnp.float32
        )
        outgoing.append(sent.astype(jnp.bfloat16))
    incoming = jnp.zeros_like(own)
    for offset in range(1, OFFSETS + 1):
        arrived = passed_along(outgoing[offset - 1], "occ", offset)
        incoming = incoming + arrived.astype(jnp.float32)
    gamma = (own + incoming).astype(jnp.bfloat16)[None]
    slabs = lax.all_to_all(gamma, "occ", split_axis=1, concat_axis=0, tiled=True)
    return jnp.einsum("ipa,ma->pim", slabs, coeffs, preferred_element_type=jnp.float32).astype(
        jnp.bfloat16
    )


LANES = 128
ROWS = 128
CHUNK = ROWS // 2

BACK_STEPS = 2
DEPTH = 3

ITEMS = (
    ((0, 0, 0, 1, 1, 1), (0, 0, 0, 1, 1, 1)),
    ((2, 0, 3, 0, 0, 0), (2, 1, 3, 1, 0, 0)),
    ((5, 0, 5, 1, 0, 0), (2, 2, 3, 2, 0, 0)),
    ((2, 0, 2, 1, 4, 0), (2, 2, 2, 3, 4, 0)),
    ((2, 0, 2, 1, 3, 1), (4, 0, 4, 1, 5, 1)),
    ((2, 3, 3, 3, 0, 0), (5, 2, 5, 3, 0, 0)),
    ((6, 0, 7, 0, 0, 0), (6, 0, 7, 0, 4, 0)),
    ((2, 0, 2, 1, 5, 0), (2, 2, 2, 3, 5, 0)),
    ((6, 1, 7, 1, 0, 0), (6, 1, 7, 1, 4, 0)),
    ((6, 2, 7, 2, 0, 0), (6, 2, 7, 2, 4, 0)),
    ((6, 0, 6, 1, 3, 0), (6, 2, 6, 3, 3, 0)),
    ((6, 3, 7, 3, 0, 0), (6, 3, 7, 3, 4, 0)),
    ((6, 0, 6, 1, 7, 1), (6, 0, 6, 1, 7, 1)),
)
PASSED = (4, 6, 8, 9)
FAR = (6, 8, 9, 11)


def flipped(a, b):
    bits = [(a // w % 2 + b // w % 2) % 2 * w for w in (1, 2, 4)]
    return bits[0] + bits[1] + bits[2]


def octal(packed, n):
    return lax.shift_right_logical(packed, jnp.int32(3) * n) % 8


def pack(ua, ta, ub, tb, v):
    return ua + 8 * ta + 64 * ub + 512 * tb + 4096 * v


def unpack(code):
    return tuple(octal(code, k) for k in range(5))


def gathered_kernel(
    mine_ref, energy_hbm, vir_hbm, out_ref,
    blocks, slabs, total, wide, pick, vcol, held_a, held_b, energy_ref, vir_ref,
    local_sem, small_sem, own_sem, fwd_sem, sib_sem, recv_sem, give_sem, take_sem,
):
    me = lax.axis_index("occ")
    parity = me % 2
    count = blocks.shape[0]
    virtuals, depth = mine_ref.shape
    width = total.shape[1]
    window = pick.shape[1]
    steps = virtuals // ROWS
    chunks = virtuals // CHUNK
    half = virtuals // 2
    rounds = len(ITEMS)
    first = me * width
    lead = pl.multiple_of(first // LANES * LANES, LANES)
    skip = first % LANES

    def rows_of(q):
        return pl.ds(pl.multiple_of(q * CHUNK, CHUNK), CHUNK)

    def local(q):
        return pltpu.make_async_copy(
            mine_ref.at[rows_of(q)], blocks.at[me, rows_of(q)], local_sem.at[q]
        )

    energy_copy = pltpu.make_async_copy(energy_hbm, energy_ref, small_sem.at[0])
    vir_copy = pltpu.make_async_copy(vir_hbm, vir_ref, small_sem.at[1])

    barrier = pltpu.get_barrier_semaphore()
    for bit in (1, 2, 4):
        pl.semaphore_signal(
            barrier, inc=1, device_id={"occ": flipped(me, bit)},
            device_id_type=pl.DeviceIdType.MESH,
        )

    @pl.loop(0, chunks)
    def _(q):
        local(q).start()

    energy_copy.start()
    vir_copy.start()
    pl.semaphore_wait(barrier, 3)

    def send(label, q, bit, send_sem):
        place = blocks.at[flipped(me, label), rows_of(q)]
        return pltpu.make_async_remote_copy(
            src_ref=place,
            dst_ref=place,
            send_sem=send_sem,
            recv_sem=recv_sem.at[flipped(label, bit), q],
            device_id={"occ": flipped(me, bit)},
            device_id_type=pl.DeviceIdType.MESH,
        )

    def own_send(q, axis):
        return send(0, q, 2 + 2 * axis, own_sem.at[axis, q])

    def far_send(q, label):
        return send(label, q, 6 - label, fwd_sem.at[q])

    def sib_send(q, label):
        return send(label, q, 1, sib_sem.at[label // 2, q])

    def arrived(label, q):
        place = blocks.at[flipped(me, label), rows_of(q)]
        pltpu.make_async_copy(place, place, recv_sem.at[label, q]).wait()

    def give(n):
        return pltpu.make_async_remote_copy(
            src_ref=held_a.at[n],
            dst_ref=held_b.at[n],
            send_sem=give_sem.at[n],
            recv_sem=take_sem.at[n],
            device_id={"occ": flipped(me, 1)},
            device_id_type=pl.DeviceIdType.MESH,
        )

    def taken(n):
        place = held_b.at[n]
        pltpu.make_async_copy(place, place, take_sem.at[n]).wait()

    def next_sends(q):
        @pl.when(q < chunks)
        def _():
            own_send(q, 0).start()
            own_send(q, 1).start()

        @pl.when(q >= chunks)
        def _():
            far_send(2 * (q - chunks), 2).start()
            far_send(2 * (q - chunks) + 1, 4).start()

    for q in range(DEPTH):
        local(q).wait()
        own_send(q, 0).start()
        own_send(q, 1).start()
        sib_send(q, 0).start()

    @pl.loop(DEPTH, chunks)
    def _(q):
        local(q).wait()
        sib_send(q, 0).start()

    energy_copy.wait()
    vir_copy.wait()
    total[...] = jnp.zeros_like(total)
    for n in range(3):
        held_a[n] = jnp.zeros(held_a.shape[1:], held_a.dtype)
        held_b[n] = jnp.zeros(held_b.shape[1:], held_b.dtype)
    column = lax.broadcasted_iota(jnp.int32, (width, window), 1)
    row = lax.broadcasted_iota(jnp.int32, (width, window), 0)
    pick[...] = jnp.where(column == row + skip, 1.0, 0.0).astype(jnp.bfloat16)
    for t in range(steps):
        part = vir_ref[:, t * ROWS:(t + 1) * ROWS]
        vcol[t * ROWS:(t + 1) * ROWS, :] = jnp.broadcast_to(part, (ROWS, ROWS)).T

    def rows_at(t):
        return pl.ds(pl.multiple_of(t * ROWS, ROWS), ROWS)

    def turn_all(label):
        u = flipped(me, label)
        slabs[u] = lax.dot_general(
            pick[...], blocks[u, :, pl.ds(lead, window)], (((1,), (1,)), ((), ())),
            preferred_element_type=jnp.float32,
        ).astype(jnp.bfloat16)

    def turn(la, lb, t):
        ua, ub = flipped(me, la), flipped(me, lb)
        both = jnp.concatenate(
            [blocks[ua, rows_at(t), pl.ds(lead, window)], blocks[ub, rows_at(t), pl.ds(lead, window)]],
            axis=0,
        )
        moved = lax.dot_general(
            pick[...], both, (((1,), (1,)), ((), ())), preferred_element_type=jnp.float32
        ).astype(jnp.bfloat16)
        slabs[ua, :, rows_at(t)] = moved[:, :ROWS]
        slabs[ub, :, rows_at(t)] = moved[:, ROWS:]

    def amps_of(code, n):
        ua, ta, ub, tb, v = unpack(code)
        some = jnp.concatenate([blocks[ua, rows_at(ta), :], blocks[ub, rows_at(tb), :]], axis=0)
        level = jnp.concatenate(
            [energy_ref[ua] - vir_ref[:, rows_at(ta)], energy_ref[ub] - vir_ref[:, rows_at(tb)]],
            axis=1,
        ) + energy_ref[v]
        for h in range(2):
            rows = slice(h * half, (h + 1) * half)
            kmat = lax.dot_general(
                blocks[v, rows, :], some, (((1,), (1,)), ((), ())),
                preferred_element_type=jnp.float32,
            )
            held_a[n, rows, :] = (kmat / (level - vcol[rows, 0:1])).astype(jnp.bfloat16)

    def gather(code, held):
        ua, ta, ub, tb, v = unpack(code)
        left = jnp.concatenate([slabs[ua, :, rows_at(ta)], slabs[ub, :, rows_at(tb)]], axis=1)
        both = jnp.dot(slabs[v], held[...], preferred_element_type=jnp.float32)
        other = lax.dot_general(
            left, held[...], (((1,), (1,)), ((), ())), preferred_element_type=jnp.float32
        )
        total[ua, :, rows_at(ta)] += both[:, :ROWS]
        total[ub, :, rows_at(tb)] += both[:, ROWS:]
        total[v] += other

    def gather_all(codes, n):
        gather(codes[0], held_a.at[n])
        gather(codes[1], held_b.at[n])
        gather(codes[2], held_a.at[n + 1])
        gather(codes[3], held_b.at[n + 1])

    place_of = jnp.int32(0)
    for label in range(8):
        place_of = place_of + flipped(me, label) * 8 ** label

    def codes_of(j):
        codes = []
        for s in range(2):
            packed = jnp.int32(0)
            for k in range(rounds):
                row = ITEMS[k][s]
                packed = jnp.where(j == k, sum(x << (3 * c) for c, x in enumerate(row)), packed)
            lu, ta, lw, tb, lv, same = (octal(packed, c) for c in range(6))
            turned_by = same * parity
            ua, ub, v = (
                octal(place_of, x) for x in (lu + turned_by, lw + turned_by, lv - turned_by)
            )
            codes.append(pack(ua, ta + 2 * turned_by, ub, tb + 2 * turned_by, v))
            swap = 1 - same
            shift = 2 * same * (1 - 2 * parity)
            codes.append(
                pack(
                    ua + swap * (1 - 2 * (ua % 2)), ta + 2 * turned_by + shift,
                    ub + swap * (1 - 2 * (ub % 2)), tb + 2 * turned_by + shift,
                    v + swap * (1 - 2 * (v % 2)),
                )
            )
        return tuple(codes)

    @pl.loop(0, chunks)
    def _(q):
        arrived(1, q)

    turn_all(0)
    turn_all(1)

    def near_pass(t):
        for k in (0, 1):
            q = 2 * t + k
            arrived(2, q)
            arrived(4, q)
            next_sends(q + DEPTH)
            sib_send(q, 2).start()
            sib_send(q, 4).start()

    def near_take(t):
        turn(2, 4, t)
        for k in (0, 1):
            arrived(3, 2 * t + k)
            arrived(5, 2 * t + k)
        turn(3, 5, t)

    def pass_far(t):
        for k in (0, 1):
            q = 2 * t + k
            arrived(6, q)
            sib_send(q, 6).start()

        @pl.when(chunks + t + DEPTH < chunks + chunks // 2)
        def _():
            next_sends(chunks + t + DEPTH)

    def far_event(t):
        for k in (0, 1):
            arrived(7, 2 * t + k)
        turn(6, 7, t)

    def at(table, j, event):
        step = jnp.int32(-1)
        for t, k in enumerate(table):
            step = jnp.where(j == k, t, step)

        @pl.when(step >= 0)
        def _():
            event(step)

    def body(j, carry):
        last, mid, now = carry

        @pl.when(j == 1)
        def _():
            near_pass(0)
            near_take(0)

        @pl.when(j <= steps - 1)
        def _():
            near_pass(j)

        @pl.when((j <= steps - 2) | (j == steps))
        def _():
            near_take(j - j // steps)

        at(FAR, j, far_event)
        amps_of(now[0], 2 * j + 2)
        amps_of(now[2], 2 * j + 3)
        give(2 * j + 2).start()
        give(2 * j + 3).start()
        at(PASSED, j, pass_far)

        @pl.when(j >= 2)
        def _():
            taken(2 * j - 1)

        @pl.when(j >= 3)
        def _():
            taken(2 * j - 2)

        gather_all(last, 2 * j - 2)
        return mid, now, codes_of(j + 1)

    front = codes_of(jnp.int32(0))
    amps_of(front[2], 3)
    give(3).start()
    final = rounds - 1
    last, mid, now = lax.fori_loop(1, final, body, (front, front, codes_of(jnp.int32(1))))
    amps_of(now[0], 2 * final + 2)
    give(2 * final + 2).start()
    taken(2 * final - 2)
    taken(2 * final - 1)
    gather_all(last, 2 * final - 2)
    taken(2 * final)
    taken(2 * final + 1)
    gather_all(mid, 2 * final)
    gather(now[0], held_a.at[2 * final + 2])

    def spread(label):
        u = flipped(me, label)
        for c in range(virtuals // LANES):
            wide[c, pl.ds(u, width, count), :] = total[u, :, c * LANES:(c + 1) * LANES]

    for label in range(6):
        spread(label)
    taken(2 * final + 2)
    gather(now[1], held_b.at[2 * final + 2])
    for label in (6, 7):
        spread(label)
    for c in range(virtuals // LANES):
        out_ref[:, c * LANES:(c + 1) * LANES] = wide[c].astype(jnp.bfloat16)

    @pl.loop(3, 2 * rounds + 1)
    def _(n):
        give(n).wait_send()

    @pl.loop(0, steps)
    def _(t):
        for k in (0, 1):
            q = 2 * t + k
            own_send(q, 0).wait_send()
            own_send(q, 1).wait_send()
            for label in (0, 2, 4, 6):
                sib_send(q, label).wait_send()
            far_send(q, 2 if k == 0 else 4).wait_send()


def back_kernel(gamma_ref, coeffs_ref, out_ref, done, done_sem):
    block = done.shape[1]

    def put(i):
        return pltpu.make_async_copy(
            done.at[i], out_ref.at[pl.ds(i * block, block)], done_sem.at[i]
        )

    for i in range(BACK_STEPS):
        done[i] = lax.dot_general(
            gamma_ref[i * block:(i + 1) * block, :], coeffs_ref[...], (((1,), (1,)), ((), ())),
            preferred_element_type=jnp.float32,
        ).astype(done.dtype)
        put(i).start()
    for i in range(BACK_STEPS):
        put(i).wait()


def back_of(gamma, coeffs):
    rows, virtuals = gamma.shape
    atomic = coeffs.shape[0]
    return pl.pallas_call(
        back_kernel,
        out_shape=jax.ShapeDtypeStruct((rows, atomic), jnp.bfloat16),
        in_specs=[pl.BlockSpec(memory_space=pltpu.VMEM)] * 2,
        out_specs=pl.BlockSpec(memory_space=pltpu.HBM),
        scratch_shapes=[
            pltpu.VMEM((BACK_STEPS, rows // BACK_STEPS, atomic), jnp.bfloat16),
            pltpu.SemaphoreType.DMA((BACK_STEPS,)),
        ],
        compiler_params=pltpu.CompilerParams(vmem_limit_bytes=32 * 1024 * 1024),
        cost_estimate=pl.CostEstimate(
            flops=2 * rows * virtuals * atomic, transcendentals=0,
            bytes_accessed=2 * (rows * virtuals + atomic * virtuals + rows * atomic),
        ),
    )(gamma, coeffs)


def gathered(factors, occ_energy, vir_energy, coeffs):
    _, virtuals, depth = factors.shape
    count = lax.axis_size("occ")
    width = depth // count
    window = max(
        -(-(d * width % LANES + width) // LANES) * LANES for d in range(count)
    )
    chunks = virtuals // CHUNK
    pair_flops = 2 * virtuals * virtuals * (depth + 2 * width)
    gamma = pl.pallas_call(
        gathered_kernel,
        out_shape=jax.ShapeDtypeStruct((count * width, virtuals), jnp.bfloat16),
        in_specs=[pl.BlockSpec(memory_space=pltpu.HBM)] * 3,
        out_specs=pl.BlockSpec(memory_space=pltpu.VMEM),
        scratch_shapes=[
            pltpu.VMEM((count, virtuals, depth), jnp.bfloat16),
            pltpu.VMEM((count, width, virtuals), jnp.bfloat16),
            pltpu.VMEM((count, width, virtuals), jnp.float32),
            pltpu.VMEM((virtuals // LANES, count * width, LANES), jnp.float32),
            pltpu.VMEM((width, window), jnp.bfloat16),
            pltpu.VMEM((virtuals, ROWS), jnp.float32),
            pltpu.VMEM((2 * len(ITEMS) + 1, virtuals, 2 * ROWS), jnp.bfloat16),
            pltpu.VMEM((2 * len(ITEMS) + 1, virtuals, 2 * ROWS), jnp.bfloat16),
            pltpu.SMEM((count,), jnp.float32),
            pltpu.VMEM((1, virtuals), jnp.float32),
            pltpu.SemaphoreType.DMA((chunks,)),
            pltpu.SemaphoreType.DMA((2,)),
            pltpu.SemaphoreType.DMA((2, chunks)),
            pltpu.SemaphoreType.DMA((chunks,)),
            pltpu.SemaphoreType.DMA((4, chunks)),
            pltpu.SemaphoreType.DMA((8, chunks)),
            pltpu.SemaphoreType.DMA((2 * len(ITEMS) + 1,)),
            pltpu.SemaphoreType.DMA((2 * len(ITEMS) + 1,)),
        ],
        compiler_params=pltpu.CompilerParams(
            collective_id=0, has_side_effects=True, vmem_limit_bytes=int(52 * 1024 * 1024)
        ),
        cost_estimate=pl.CostEstimate(
            flops=count * OFFSETS * pair_flops, bytes_accessed=count * virtuals * depth * 2,
            transcendentals=0,
        ),
    )(
        factors[0],
        pltpu.with_memory_space_constraint(occ_energy, pltpu.HBM),
        pltpu.with_memory_space_constraint(vir_energy[None], pltpu.HBM),
    )
    back = back_of(gamma, coeffs)
    return back.reshape(width, count, coeffs.shape[0])


def fits(count, virtuals, depth):
    width = depth // count
    return (
        count == 8
        and count * OFFSETS == 2 * len(ITEMS) - 2
        and virtuals == 4 * ROWS
        and depth % (LANES * 2) == 0
        and width % 32 == 0
    )


def either(factors, occ_energy, vir_energy, coeffs):
    if fits(lax.axis_size("occ"), factors.shape[1], factors.shape[2]):
        return gathered(factors, occ_energy, vir_energy, coeffs)
    return on_device(factors, occ_energy, vir_energy, coeffs)


def solution(mesh):
    return jax.shard_map(
        either,
        mesh=mesh,
        in_specs=(P(("frag", "occ"), None, None), P("frag"), P("frag"), P("frag", None)),
        out_specs=P("occ", "frag", None),
        check_vma=False,
    )
```
